16 devices in a mesh: dp: 2 (over y, z), tp: 8 (over x, core).
Axes of the slice: x: 4, y: 2, z: 1, core: 2. Of those that a mesh axis runs over, the one named last changes fastest.
The devices are a block of a 4x4x8 slice.
Arguments:
- x: bfloat16 [8192, 2048], P(('dp', 'tp')), parts along dimension 0
- dy: bfloat16 [8192, 2048], P(('dp', 'tp')), parts along dimension 0
- pre: bfloat16 [8192, 8192], P('dp', 'tp'), parts along dimension 0
- w_in: bfloat16 [2048, 8192], P(None, 'tp')
- w_down: bfloat16 [8192, 2048], P('tp')
Outputs:
- output 1: bfloat16 [8192, 2048], P(('dp', 'tp')), parts along dimension 0
- output 2: bfloat16 [4096, 8192], P('dp', 'tp'), parts along dimension 0
- output 3: bfloat16 [16384, 2048], P(('dp', 'tp')), parts along dimension 0
There are 2 independent parts. The reference program is written for one: setup_inputs(seed, part) draws one part's arguments, and reference() takes and returns one part's arrays. A program takes and returns all parts, laid end to end along the dimension named above; an argument that names none is the same for every part.
All inputs are finite; a program needn't handle non-finite values.
Results may differ from the reference program's by a relative error of at most 0.012.
Values are sent between devices in bfloat16 or wider.
A program may use at most 768 MiB of HBM per device.

```python
import jax
import jax.numpy as jnp

ROWS = 4096
D = 2048
FF = 8192


def act(pre):
    return jax.nn.gelu(pre)


def setup_inputs(seed: int = 0, part: int = 0) -> dict:
    kx, ky, ka, ki, kd = jax.random.split(jax.random.key(seed), 5)
    kx, ky, ka = (jax.random.fold_in(k, part) for k in (kx, ky, ka))
    drawn = {
        "x": jax.random.normal(kx, (ROWS, D), jnp.float32),
        "dy": jax.random.normal(ky, (ROWS, D), jnp.float32),
        "pre": jax.random.normal(ka, (ROWS, FF), jnp.float32),
        "w_in": jax.random.normal(ki, (D, FF), jnp.float32) * D**-0.5,
        "w_down": jax.random.normal(kd, (FF, D), jnp.float32) * FF**-0.5,
    }
    return {k: v.astype(jnp.bfloat16) for k, v in drawn.items()}


def reference(x, dy, pre, w_in, w_down):
    hidden, back = jax.vjp(act, pre.astype(jnp.float32))
    d_hidden = jnp.dot(dy, w_down.T, preferred_element_type=jnp.float32)
    d_pre = back(d_hidden)[0].astype(jnp.bfloat16)
    dx = jnp.dot(d_pre, w_in.T, preferred_element_type=jnp.float32)
    dw_in = jnp.dot(x.T, d_pre, preferred_element_type=jnp.float32)
    dw_down = jnp.dot(hidden.astype(jnp.bfloat16).T, dy, preferred_element_type=jnp.float32)
    return tuple(g.astype(jnp.bfloat16) for g in (dx, dw_in, dw_down))
```

```python
import functools

import jax
import jax.numpy as jnp
from jax import lax
from jax.experimental import pallas as pl
from jax.experimental.pallas import tpu as pltpu
from jax.sharding import PartitionSpec as P

MESH = pl.DeviceIdType.MESH
F32, BF16 = jnp.float32, jnp.bfloat16
CORES = 2
PAIRS = 8
PIECES = 4
NT = (((1,), (1,)), ((), ()))
TN = (((0,), (0,)), ((), ()))
DY, X = 0, 1
VMEM_LIMIT = 53 * 2**20


def gelu_and_slope(p):
    c = 0.7978845608028654
    sq = p * p
    t = jnp.tanh(c * (p + 0.044715 * (sq * p)))
    cdf = 0.5 * (1.0 + t)
    slope = cdf + (0.5 * p) * (1.0 - t * t) * (c * (1.0 + 0.134145 * sq))
    return p * cdf, slope


def kernel(
    n, x, dy, pre, w_in, w_down,
    dx, dw_in, dw_down, x_all, dy_all, rs_pair, rs_ring,
    acc_in, acc_down, dpre, stash, st_ring, rows_buf, pre_buf, hid, tmp, chain_buf,
    ring_s, ring_r, pair_s, pair_r, rsp_s, rsp_r, rsg_s, rsg_r, ch_s, ch_r, w_sem, pre_sem, ld_sem,
):
    wi, wd, st_pair = dw_in, dw_down, dx
    me = lax.axis_index("tp")
    core = lax.rem(me, CORES)
    chip = me // CORES
    chips = n // CORES
    right = lax.rem(me + CORES, n)
    left = lax.rem(me + n - CORES, n)
    partner = me + 1 - 2 * core
    size, ff = x.shape[0], pre.shape[1]
    d = x.shape[1]
    half = size // 2
    piece = half // PIECES

    def place(i):
        q, r = i // 2, i % 2
        odd = ((q + 1) // 2) % 2
        off = odd * (chips - 1 + 2 * r) + 2 * (q // 3)
        turned = (q // 2) * (1 - q // 3)
        return lax.rem(chip + off, chips), r + turned * (1 - 2 * r)

    def at(ref, shard, h):
        return ref.at[shard, pl.ds(pl.multiple_of(h * half, half), half)]

    def of_core(ref, i, k):
        c, h = place(i)
        return at(ref, c * CORES + k, h)

    own = (dy, x)
    gathered = (dy_all, x_all)

    def own_half(w, h):
        return own[w].at[pl.ds(h * half, half)]

    def remote(src, dst, s, r, dev):
        return pltpu.make_async_remote_copy(
            src_ref=src, dst_ref=dst, send_sem=s, recv_sem=r, device_id={"tp": dev}, device_id_type=MESH
        )

    def ring_own(w, j):
        h = {2: 0, 3: 1, 4: 1, 5: 0}[j]
        return remote(own_half(w, h), at(gathered[w], me, h), ring_s.at[w, j], ring_r.at[w, j], right if j % 2 == 0 else left)

    def ring_relay(w, j):
        ref = of_core(gathered[w], j - 4, core)
        return remote(ref, ref, ring_s.at[w, j], ring_r.at[w, j], right if j % 2 == 0 else left)

    def ring_send(w, j):
        return ring_own(w, j) if j < 6 else ring_relay(w, j)

    def ring_got(w, j):
        ref = of_core(gathered[w], j, core)
        return remote(ref, ref, ring_s.at[w, j], ring_r.at[w, j], right)

    def to_partner(w, j):
        src = own_half(w, j) if j < 2 else of_core(gathered[w], j, core)
        return remote(src, of_core(gathered[w], j, core), pair_s.at[w, j], pair_r.at[w, j], partner)

    def from_partner(w, j):
        ref = of_core(gathered[w], j, 1 - core)
        return remote(ref, ref, pair_s.at[w, j], pair_r.at[w, j], partner)

    def service(w, j):
        ring_got(w, j).wait_recv()
        if j < 4:
            ring_relay(w, j + 4).start()
        to_partner(w, j).start()

    def load(src, dst, sem):
        c = pltpu.make_async_copy(src, dst, sem)
        c.start()
        return c

    def load_rows(w, j):
        from_partner(w, j).wait_recv()
        load(of_core(gathered[w], j, 1 - core), rows_buf.at[pl.ds(0, half)], ld_sem.at[0])
        c, h = place(j)

        @pl.when(j < 2)
        def _():
            load(own[w].at[pl.ds(pl.multiple_of(h * half, half), half)], rows_buf.at[pl.ds(half, half)], ld_sem.at[1])

        @pl.when(j >= 2)
        def _():
            load(of_core(gathered[w], j, core), rows_buf.at[pl.ds(half, half)], ld_sem.at[1])

        for b in range(2):
            pltpu.make_async_copy(rows_buf.at[pl.ds(0, half)], rows_buf.at[pl.ds(b * half, half)], ld_sem.at[b]).wait()

    def pre_load(j, b):
        c, h = place(j)
        where = (1 - core) if b == 0 else core
        start = pl.multiple_of((c * CORES + where) * size + h * half, half)
        return pltpu.make_async_copy(
            pre.at[pl.ds(start, half)], pre_buf.at[j % 2, pl.ds(b * half, half)], pre_sem.at[j % 2, b]
        )

    def pair_sum(j):
        return remote(st_pair.at[pl.ds(pl.multiple_of(j % 2 * half, half), half)], rs_pair.at[j], rsp_s.at[j], rsp_r.at[j], partner)

    def ring_sum(j):
        dev = lax.rem(me + n - CORES + 2 * CORES * (j % 2), n)
        return remote(st_ring.at[j - 4], rs_ring.at[j - 4], rsg_s.at[j - 4], rsg_r.at[j - 4], dev)

    def chain_send(b, q):
        ref = (b, pl.ds(q * piece, piece))
        return remote(st_ring.at[ref], chain_buf.at[ref], ch_s.at[b, q], ch_r.at[b, q], left if b == 0 else right)

    barrier = pltpu.get_barrier_semaphore()
    for dev in (left, right, partner):
        pl.semaphore_signal(barrier, inc=1, device_id={"tp": dev}, device_id_type=MESH)
    pl.semaphore_wait(barrier, 3)

    for j in (2, 3, 4, 5):
        ring_own(DY, j).start()
    for j in (0, 1):
        to_partner(DY, j).start()
    for b in range(2):
        pre_load(0, b).start()
    load(w_down, wd, w_sem.at[0])
    load(w_in, wi, w_sem.at[1])

    @pl.loop(0, ff, step=64)
    def _(r):
        acc_down[pl.ds(pl.multiple_of(r, 64), 64)] = jnp.zeros((64, d), F32)

    @pl.loop(0, d, step=128)
    def _(r):
        acc_in[pl.ds(pl.multiple_of(r, 128), 128)] = jnp.zeros((128, ff), F32)

    pltpu.make_async_copy(w_down, wd, w_sem.at[0]).wait()
    pltpu.make_async_copy(w_in, wi, w_sem.at[1]).wait()

    tile = 256

    @pl.loop(0, PAIRS)
    def _(i):
        slot = i % 2

        @pl.when(i == 2)
        def _():
            service(DY, 2)
            service(DY, 3)
            ring_own(X, 2).start()
            ring_own(X, 3).start()
            to_partner(X, 0).start()
            to_partner(X, 1).start()

        @pl.when(i == 4)
        def _():
            service(DY, 4)
            service(DY, 5)

        @pl.when(i == 6)
        def _():
            service(DY, 6)
            service(DY, 7)
            ring_own(X, 4).start()
            ring_own(X, 5).start()

        @pl.when(i < PAIRS - 1)
        def _():
            for b in range(2):
                pre_load(i + 1, b).start()

        load_rows(DY, i)
        for b in range(2):
            pre_load(i, b).wait()

        @pl.loop(0, ff, step=tile)
        def _(f):
            fs = pl.ds(pl.multiple_of(f, tile), tile)
            dh = lax.dot_general(rows_buf[...], wd[fs, :], NT, preferred_element_type=F32)
            h, slope = gelu_and_slope(pre_buf[slot, :, fs].astype(F32))
            dpre[i, :, fs] = (dh * slope).astype(BF16)
            hid[:, fs] = h.astype(BF16)

        @pl.when(i >= 2)
        def _():
            pair_sum(i - 2).wait_send()

        @pl.loop(0, d, step=2 * tile)
        def _(c):
            cs = pl.ds(pl.multiple_of(c, 2 * tile), 2 * tile)
            o = lax.dot_general(dpre[i, 0:half, :], wi[cs, :], NT, preferred_element_type=F32)
            st_pair[pl.ds(pl.multiple_of(slot * half, half), half), cs] = o.astype(BF16)

        pair_sum(i).start()

        @pl.loop(0, ff, step=tile)
        def _(f):
            fs = pl.ds(pl.multiple_of(f, tile), tile)

            for c in range(0, d, 2 * tile):
                acc_down[fs, c : c + 2 * tile] += lax.dot_general(
                    hid[:, fs], rows_buf[:, c : c + 2 * tile], TN, preferred_element_type=F32
                )

        pair_sum(i).wait_recv()
        load(rs_pair.at[i], tmp, ld_sem.at[0]).wait()

        def mine(c):
            cs = pl.ds(pl.multiple_of(c, 2 * tile), 2 * tile)
            o = lax.dot_general(dpre[i, half : 2 * half, :], wi[cs, :], NT, preferred_element_type=F32)
            return cs, o + tmp[:, cs].astype(F32)

        @pl.when(i < 4)
        def _():
            @pl.loop(0, d, step=2 * tile)
            def _(c):
                cs, o = mine(c)
                stash[i, :, cs] = o

        @pl.when(i >= 4)
        def _():
            @pl.loop(0, d, step=2 * tile)
            def _(c):
                cs, o = mine(c)
                st_ring[i - 4, :, cs] = o.astype(BF16)

            ring_sum(i).start()

    service(X, 2)
    service(X, 3)

    for b in range(2):
        pair_sum(PAIRS - 2 + b).wait_send()

    @pl.loop(0, ff, step=32)
    def _(r):
        rs = pl.ds(pl.multiple_of(r, 32), 32)
        dw_down[rs] = acc_down[rs].astype(BF16)

    def chain(b):
        ring_sum(6 + b).wait_recv()
        load(rs_ring.at[2 + b], tmp, ld_sem.at[0]).wait()
        ring_sum(4 + b).wait_send()

        @pl.loop(0, half, step=32)
        def _(r):
            rs = pl.ds(pl.multiple_of(r, 32), 32)
            st_ring[b, rs] = (stash[2 + b, rs] + tmp[rs].astype(F32)).astype(BF16)

        for q in range(PIECES):
            chain_send(b, q).start()

    def direct(b):
        ring_sum(4 + b).wait_recv()
        load(rs_ring.at[b], tmp, ld_sem.at[0]).wait()

        @pl.loop(0, half, step=32)
        def _(r):
            rs = pl.ds(pl.multiple_of(r, 32), 32)
            stash[1 - b, rs] += tmp[rs].astype(F32)

    @pl.loop(0, PAIRS)
    def _(i):
        @pl.when(i == 4)
        def _():
            direct(0)
            direct(1)
            chain(0)
            chain(1)
            service(X, 4)
            service(X, 5)

        @pl.when(i == 6)
        def _():
            service(X, 6)
            service(X, 7)

        load_rows(X, i)

        @pl.loop(0, d, step=tile)
        def _(c):
            cs = pl.ds(pl.multiple_of(c, tile), tile)

            for f in range(0, ff, 2 * tile):
                acc_in[cs, f : f + 2 * tile] += lax.dot_general(
                    rows_buf[:, cs], dpre[i, :, f : f + 2 * tile], TN, preferred_element_type=F32
                )

    @pl.loop(0, d, step=64)
    def _(r):
        rs = pl.ds(pl.multiple_of(r, 64), 64)
        dw_in[rs] = acc_in[rs].astype(BF16)

    for q in range(PIECES):
        for b in range(2):
            chain_send(b, q).wait_recv()
            rs = pl.ds(q * piece, piece)
            dx[pl.ds(b * half + q * piece, piece)] = (stash[b, rs] + chain_buf[b, rs].astype(F32)).astype(BF16)

    for w in (DY, X):
        for j in range(2, PAIRS):
            ring_send(w, j).wait_send()
        for j in range(PAIRS):
            to_partner(w, j).wait_send()
    for j in (6, 7):
        ring_sum(j).wait_send()
    for b in range(2):
        for q in range(PIECES):
            chain_send(b, q).wait_send()


def results(*refs):
    count = len(refs) // 2
    ins, outs, sem = refs[:count], refs[count : 2 * count], refs[-1]
    copies = [pltpu.make_async_copy(a, b, sem.at[i]) for i, (a, b) in enumerate(zip(ins, outs))]
    for c in copies:
        c.start()
    for c in copies:
        c.wait()


def solution(mesh):
    n = mesh.shape["tp"]

    def step(x, dy, pre, w_in, w_down):
        (size, d), ff = x.shape, pre.shape[1]
        half = size // 2
        any_space = pl.BlockSpec(memory_space=pl.ANY)
        shapes = ((size, d), (d, ff), (ff, d))
        dma = pltpu.SemaphoreType.DMA
        outs = pl.pallas_call(
            functools.partial(kernel, n),
            out_shape=[pltpu.VMEM(s, BF16) for s in shapes]
            + [
                jax.ShapeDtypeStruct(s, BF16)
                for s in ((n, size, d), (n, size, d), (PAIRS, half, d), (4, half, d))
            ],
            in_specs=[any_space] * 5,
            out_specs=[pl.BlockSpec(memory_space=pltpu.VMEM)] * 3 + [any_space] * 4,
            scratch_shapes=[
                pltpu.VMEM((d, ff), F32),
                pltpu.VMEM((ff, d), F32),
                pltpu.VMEM((PAIRS, size, ff), BF16),
                pltpu.VMEM((4, half, d), F32),
                pltpu.VMEM((4, half, d), BF16),
                pltpu.VMEM((size, d), BF16),
                pltpu.VMEM((2, size, ff), BF16),
                pltpu.VMEM((size, ff), BF16),
                pltpu.VMEM((half, d), BF16),
                pltpu.VMEM((2, half, d), BF16),
                dma((2, PAIRS)), dma((2, PAIRS)), dma((2, PAIRS)), dma((2, PAIRS)),
                dma((PAIRS,)), dma((PAIRS,)), dma((4,)), dma((4,)), dma((2, PIECES)), dma((2, PIECES)),
                dma((2,)), dma((2, 2)), dma((2,)),
            ],
            compiler_params=pltpu.CompilerParams(collective_id=0, has_side_effects=True, vmem_limit_bytes=VMEM_LIMIT),
            name="mlp_backward",
        )(x, dy, pre, w_in, w_down)
        return tuple(
            pl.pallas_call(
                results,
                out_shape=[jax.ShapeDtypeStruct(s, BF16) for s in shapes],
                in_specs=[pl.BlockSpec(memory_space=pltpu.VMEM)] * 3,
                out_specs=[any_space] * 3,
                scratch_shapes=[dma((3,))],
                compiler_params=pltpu.CompilerParams(vmem_limit_bytes=2**20),
                name="results",
            )(*(pltpu.with_memory_space_constraint(o, pltpu.VMEM) for o in outs[:3]))
        )

    rows = P(("dp", "tp"), None)
    return jax.shard_map(
        step,
        mesh=mesh,
        in_specs=(rows, rows, P("dp", "tp"), P(None, "tp"), P("tp", None)),
        out_specs=(rows, P("dp", "tp"), rows),
        check_vma=False,
    )
```

```python
import functools

import jax
import jax.numpy as jnp
from jax import lax
from jax.experimental import pallas as pl
from jax.experimental.pallas import tpu as pltpu
from jax.sharding import PartitionSpec as P

MESH = pl.DeviceIdType.MESH
F32, BF16 = jnp.float32, jnp.bfloat16
CORES = 2
PAIRS = 8
PIECES = 2
NT = (((1,), (1,)), ((), ()))
TN = (((0,), (0,)), ((), ()))
DY, X = 0, 1
VMEM_LIMIT = 53 * 2**20


def gelu_and_slope(p):
    c = 0.7978845608028654
    sq = p * p
    t = jnp.tanh(c * (p + 0.044715 * (sq * p)))
    cdf = 0.5 * (1.0 + t)
    slope = cdf + (0.5 * p) * (1.0 - t * t) * (c * (1.0 + 0.134145 * sq))
    return p * cdf, slope


def kernel(
    n, x, dy, pre, w_in, w_down,
    dx, dw_in, dw_down, x_all, dy_all, rs_pair, rs_ring,
    acc_in, acc_down, dpre, stash, st_ring, rows_buf, pre_buf, hid, tmp, chain_buf,
    ring_s, ring_r, pair_s, pair_r, rsp_s, rsp_r, rsg_s, rsg_r, ch_s, ch_r, w_sem, pre_sem, ld_sem,
):
    wi, wd, st_pair = dw_in, dw_down, dx
    me = lax.axis_index("tp")
    core = lax.rem(me, CORES)
    chip = me // CORES
    chips = n // CORES
    right = lax.rem(me + CORES, n)
    left = lax.rem(me + n - CORES, n)
    partner = me + 1 - 2 * core
    size, ff = x.shape[0], pre.shape[1]
    d = x.shape[1]
    half = size // 2
    piece = half // PIECES

    def place(i):
        q, r = i // 2, i % 2
        odd = ((q + 1) // 2) % 2
        off = odd * (chips - 1 + 2 * r) + 2 * (q // 3)
        turned = (q // 2) * (1 - q // 3)
        return lax.rem(chip + off, chips), r + turned * (1 - 2 * r)

    def at(ref, shard, h):
        return ref.at[shard, pl.ds(pl.multiple_of(h * half, half), half)]

    def of_core(ref, i, k):
        c, h = place(i)
        return at(ref, c * CORES + k, h)

    own = (dy, x)
    gathered = (dy_all, x_all)

    def own_half(w, h):
        return own[w].at[pl.ds(h * half, half)]

    def remote(src, dst, s, r, dev):
        return pltpu.make_async_remote_copy(
            src_ref=src, dst_ref=dst, send_sem=s, recv_sem=r, device_id={"tp": dev}, device_id_type=MESH
        )

    def ring_own(w, j):
        h = {2: 0, 3: 1, 4: 1, 5: 0}[j]
        return remote(own_half(w, h), at(gathered[w], me, h), ring_s.at[w, j], ring_r.at[w, j], right if j % 2 == 0 else left)

    def ring_relay(w, j):
        ref = of_core(gathered[w], j - 4, core)
        return remote(ref, ref, ring_s.at[w, j], ring_r.at[w, j], right if j % 2 == 0 else left)

    def ring_send(w, j):
        return ring_own(w, j) if j < 6 else ring_relay(w, j)

    def ring_got(w, j):
        ref = of_core(gathered[w], j, core)
        return remote(ref, ref, ring_s.at[w, j], ring_r.at[w, j], right)

    def to_partner(w, j):
        src = own_half(w, j) if j < 2 else of_core(gathered[w], j, core)
        return remote(src, of_core(gathered[w], j, core), pair_s.at[w, j], pair_r.at[w, j], partner)

    def from_partner(w, j):
        ref = of_core(gathered[w], j, 1 - core)
        return remote(ref, ref, pair_s.at[w, j], pair_r.at[w, j], partner)

    def service(w, j):
        ring_got(w, j).wait_recv()
        if j < 4:
            ring_relay(w, j + 4).start()
        to_partner(w, j).start()

    def load(src, dst, sem):
        c = pltpu.make_async_copy(src, dst, sem)
        c.start()
        return c

    def load_rows(w, j):
        from_partner(w, j).wait_recv()
        load(of_core(gathered[w], j, 1 - core), rows_buf.at[pl.ds(0, half)], ld_sem.at[0])
        c, h = place(j)

        @pl.when(j < 2)
        def _():
            load(own[w].at[pl.ds(pl.multiple_of(h * half, half), half)], rows_buf.at[pl.ds(half, half)], ld_sem.at[1])

        @pl.when(j >= 2)
        def _():
            load(of_core(gathered[w], j, core), rows_buf.at[pl.ds(half, half)], ld_sem.at[1])

        for b in range(2):
            pltpu.make_async_copy(rows_buf.at[pl.ds(0, half)], rows_buf.at[pl.ds(b * half, half)], ld_sem.at[b]).wait()

    def pre_load(j, b):
        c, h = place(j)
        where = (1 - core) if b == 0 else core
        start = pl.multiple_of((c * CORES + where) * size + h * half, half)
        return pltpu.make_async_copy(
            pre.at[pl.ds(start, half)], pre_buf.at[j % 2, pl.ds(b * half, half)], pre_sem.at[j % 2, b]
        )

    def pair_sum(j):
        return remote(st_pair.at[pl.ds(pl.multiple_of(j % 2 * half, half), half)], rs_pair.at[j], rsp_s.at[j], rsp_r.at[j], partner)

    def ring_sum(j):
        dev = lax.rem(me + n - CORES + 2 * CORES * (j % 2), n)
        return remote(st_ring.at[j - 4], rs_ring.at[j - 4], rsg_s.at[j - 4], rsg_r.at[j - 4], dev)

    def chain_send(b, q):
        ref = (b, pl.ds(q * piece, piece))
        return remote(st_ring.at[ref], chain_buf.at[ref], ch_s.at[b, q], ch_r.at[b, q], left if b == 0 else right)

    barrier = pltpu.get_barrier_semaphore()
    for dev in (left, right, partner):
        pl.semaphore_signal(barrier, inc=1, device_id={"tp": dev}, device_id_type=MESH)
    pl.semaphore_wait(barrier, 3)

    for j in (2, 3, 4, 5):
        ring_own(DY, j).start()
    for j in (0, 1):
        to_partner(DY, j).start()
    for b in range(2):
        pre_load(0, b).start()
    load(w_down, wd, w_sem.at[0])
    load(w_in, wi, w_sem.at[1])

    @pl.loop(0, ff, step=64)
    def _(r):
        acc_down[pl.ds(pl.multiple_of(r, 64), 64)] = jnp.zeros((64, d), F32)

    @pl.loop(0, d, step=128)
    def _(r):
        acc_in[pl.ds(pl.multiple_of(r, 128), 128)] = jnp.zeros((128, ff), F32)

    pltpu.make_async_copy(w_down, wd, w_sem.at[0]).wait()
    pltpu.make_async_copy(w_in, wi, w_sem.at[1]).wait()

    tile = 256

    @pl.loop(0, PAIRS)
    def _(i):
        slot = i % 2

        @pl.when(i == 2)
        def _():
            service(DY, 2)
            service(DY, 3)
            ring_own(X, 2).start()
            ring_own(X, 3).start()
            to_partner(X, 0).start()
            to_partner(X, 1).start()

        @pl.when(i == 4)
        def _():
            service(DY, 4)
            service(DY, 5)
            ring_own(X, 4).start()
            ring_own(X, 5).start()

        @pl.when(i == 6)
        def _():
            service(DY, 6)
            service(DY, 7)

        @pl.when(i < PAIRS - 1)
        def _():
            for b in range(2):
                pre_load(i + 1, b).start()

        load_rows(DY, i)
        for b in range(2):
            pre_load(i, b).wait()

        @pl.loop(0, ff, step=tile)
        def _(f):
            fs = pl.ds(pl.multiple_of(f, tile), tile)
            dh = lax.dot_general(rows_buf[...], wd[fs, :], NT, preferred_element_type=F32)
            h, slope = gelu_and_slope(pre_buf[slot, :, fs].astype(F32))
            dpre[i, :, fs] = (dh * slope).astype(BF16)
            hid[:, fs] = h.astype(BF16)

        @pl.when(i >= 2)
        def _():
            pair_sum(i - 2).wait_send()

        @pl.loop(0, d, step=2 * tile)
        def _(c):
            cs = pl.ds(pl.multiple_of(c, 2 * tile), 2 * tile)
            o = lax.dot_general(dpre[i, 0:half, :], wi[cs, :], NT, preferred_element_type=F32)
            st_pair[pl.ds(pl.multiple_of(slot * half, half), half), cs] = o.astype(BF16)

        pair_sum(i).start()

        @pl.loop(0, ff, step=tile)
        def _(f):
            fs = pl.ds(pl.multiple_of(f, tile), tile)

            for c in range(0, d, 2 * tile):
                acc_down[fs, c : c + 2 * tile] += lax.dot_general(
                    hid[:, fs], rows_buf[:, c : c + 2 * tile], TN, preferred_element_type=F32
                )

        pair_sum(i).wait_recv()
        load(rs_pair.at[i], tmp, ld_sem.at[0]).wait()

        def mine(c):
            cs = pl.ds(pl.multiple_of(c, 2 * tile), 2 * tile)
            o = lax.dot_general(dpre[i, half : 2 * half, :], wi[cs, :], NT, preferred_element_type=F32)
            return cs, o + tmp[:, cs].astype(F32)

        @pl.when(i < 4)
        def _():
            @pl.loop(0, d, step=2 * tile)
            def _(c):
                cs, o = mine(c)
                stash[i, :, cs] = o

        @pl.when(i >= 4)
        def _():
            @pl.loop(0, d, step=2 * tile)
            def _(c):
                cs, o = mine(c)
                st_ring[i - 4, :, cs] = o.astype(BF16)

            ring_sum(i).start()

    service(X, 2)
    service(X, 3)

    for b in range(2):
        pair_sum(PAIRS - 2 + b).wait_send()

    @pl.loop(0, ff, step=32)
    def _(r):
        rs = pl.ds(pl.multiple_of(r, 32), 32)
        dw_down[rs] = acc_down[rs].astype(BF16)

    def chain(b):
        ring_sum(6 + b).wait_recv()
        load(rs_ring.at[2 + b], tmp, ld_sem.at[0]).wait()
        ring_sum(4 + b).wait_send()

        @pl.loop(0, half, step=32)
        def _(r):
            rs = pl.ds(pl.multiple_of(r, 32), 32)
            st_ring[b, rs] = (stash[2 + b, rs] + tmp[rs].astype(F32)).astype(BF16)

        for q in range(PIECES):
            chain_send(b, q).start()

    def direct(b):
        ring_sum(4 + b).wait_recv()
        load(rs_ring.at[b], tmp, ld_sem.at[0]).wait()

        @pl.loop(0, half, step=32)
        def _(r):
            rs = pl.ds(pl.multiple_of(r, 32), 32)
            stash[1 - b, rs] += tmp[rs].astype(F32)

    @pl.loop(0, PAIRS)
    def _(i):
        @pl.when(i == 4)
        def _():
            direct(0)
            direct(1)
            chain(0)
            chain(1)
            service(X, 4)
            service(X, 5)

        @pl.when(i == 6)
        def _():
            service(X, 6)
            service(X, 7)

        load_rows(X, i)

        @pl.loop(0, d, step=tile)
        def _(c):
            cs = pl.ds(pl.multiple_of(c, tile), tile)

            for f in range(0, ff, 2 * tile):
                acc_in[cs, f : f + 2 * tile] += lax.dot_general(
                    rows_buf[:, cs], dpre[i, :, f : f + 2 * tile], TN, preferred_element_type=F32
                )

    @pl.loop(0, d, step=64)
    def _(r):
        rs = pl.ds(pl.multiple_of(r, 64), 64)
        dw_in[rs] = acc_in[rs].astype(BF16)

    for w in (DY, X):
        for j in range(2, PAIRS):
            ring_send(w, j).wait_send()
        for j in range(PAIRS):
            to_partner(w, j).wait_send()
    for j in (6, 7):
        ring_sum(j).wait_send()

    for q in range(PIECES):
        for b in range(2):
            chain_send(b, q).wait_recv()
            rs = pl.ds(q * piece, piece)
            dx[pl.ds(b * half + q * piece, piece)] = (stash[b, rs] + chain_buf[b, rs].astype(F32)).astype(BF16)

    for b in range(2):
        for q in range(PIECES):
            chain_send(b, q).wait_send()


def results(*refs):
    count = len(refs) // 2
    ins, outs, sem = refs[:count], refs[count : 2 * count], refs[-1]
    copies = []
    for a, b in zip(ins, outs):
        rows = a.shape[0] // 2
        for i in range(2):
            rs = pl.ds(i * rows, rows)
            copies.append(pltpu.make_async_copy(a.at[rs], b.at[rs], sem.at[len(copies)]))
    for c in copies:
        c.start()
    for c in copies:
        c.wait()


def solution(mesh):
    n = mesh.shape["tp"]

    def step(x, dy, pre, w_in, w_down):
        (size, d), ff = x.shape, pre.shape[1]
        half = size // 2
        any_space = pl.BlockSpec(memory_space=pl.ANY)
        shapes = ((size, d), (d, ff), (ff, d))
        dma = pltpu.SemaphoreType.DMA
        outs = pl.pallas_call(
            functools.partial(kernel, n),
            out_shape=[pltpu.VMEM(s, BF16) for s in shapes]
            + [
                jax.ShapeDtypeStruct(s, BF16)
                for s in ((n, size, d), (n, size, d), (PAIRS, half, d), (4, half, d))
            ],
            in_specs=[any_space] * 5,
            out_specs=[pl.BlockSpec(memory_space=pltpu.VMEM)] * 3 + [any_space] * 4,
            scratch_shapes=[
                pltpu.VMEM((d, ff), F32),
                pltpu.VMEM((ff, d), F32),
                pltpu.VMEM((PAIRS, size, ff), BF16),
                pltpu.VMEM((4, half, d), F32),
                pltpu.VMEM((4, half, d), BF16),
                pltpu.VMEM((size, d), BF16),
                pltpu.VMEM((2, size, ff), BF16),
                pltpu.VMEM((size, ff), BF16),
                pltpu.VMEM((half, d), BF16),
                pltpu.VMEM((2, half, d), BF16),
                dma((2, PAIRS)), dma((2, PAIRS)), dma((2, PAIRS)), dma((2, PAIRS)),
                dma((PAIRS,)), dma((PAIRS,)), dma((4,)), dma((4,)), dma((2, PIECES)), dma((2, PIECES)),
                dma((2,)), dma((2, 2)), dma((2,)),
            ],
            compiler_params=pltpu.CompilerParams(collective_id=0, has_side_effects=True, vmem_limit_bytes=VMEM_LIMIT),
            name="mlp_backward",
        )(x, dy, pre, w_in, w_down)
        return tuple(
            pl.pallas_call(
                results,
                out_shape=[jax.ShapeDtypeStruct(s, BF16) for s in shapes],
                in_specs=[pl.BlockSpec(memory_space=pltpu.VMEM)] * 3,
                out_specs=[any_space] * 3,
                scratch_shapes=[dma((6,))],
                compiler_params=pltpu.CompilerParams(vmem_limit_bytes=2**20),
                name="results",
            )(*(pltpu.with_memory_space_constraint(o, pltpu.VMEM) for o in outs[:3]))
        )

    rows = P(("dp", "tp"), None)
    return jax.shard_map(
        step,
        mesh=mesh,
        in_specs=(rows, rows, P("dp", "tp"), P(None, "tp"), P("tp", None)),
        out_specs=(rows, P("dp", "tp"), rows),
        check_vma=False,
    )
```

```python
import functools

import jax
import jax.numpy as jnp
from jax import lax
from jax.experimental import pallas as pl
from jax.experimental.pallas import tpu as pltpu
from jax.sharding import PartitionSpec as P

MESH = pl.DeviceIdType.MESH
F32, BF16 = jnp.float32, jnp.bfloat16
CORES = 2
PAIRS = 8
PIECES = 2
NT = (((1,), (1,)), ((), ()))
TN = (((0,), (0,)), ((), ()))
DY, X = 0, 1
VMEM_LIMIT = 53 * 2**20


def gelu_and_slope(p):
    c = 0.7978845608028654
    sq = p * p
    t = jnp.tanh(c * (p + 0.044715 * (sq * p)))
    cdf = 0.5 * (1.0 + t)
    slope = cdf + (0.5 * p) * (1.0 - t * t) * (c * (1.0 + 0.134145 * sq))
    return p * cdf, slope


def kernel(
    n, x, dy, pre, w_in, w_down,
    dx, dw_in, dw_down, x_all, dy_all,
    acc_in, acc_down, dpre, stash, st_ring, rows_buf, pre_buf, hid, pair_buf, ring_buf, chain_buf,
    ring_s, ring_r, pair_s, pair_r, rsp_s, rsp_r, rsg_s, rsg_r, ch_s, ch_r, w_sem, pre_sem, ld_sem,
):
    wi, wd, st_pair = dw_in, dw_down, dx
    me = lax.axis_index("tp")
    core = lax.rem(me, CORES)
    chip = me // CORES
    chips = n // CORES
    right = lax.rem(me + CORES, n)
    left = lax.rem(me + n - CORES, n)
    partner = me + 1 - 2 * core
    size, ff = x.shape[0], pre.shape[1]
    d = x.shape[1]
    half = size // 2
    piece = half // PIECES

    def place(i):
        q, r = i // 2, i % 2
        odd = ((q + 1) // 2) % 2
        off = odd * (chips - 1 + 2 * r) + 2 * (q // 3)
        turned = (q // 2) * (1 - q // 3)
        return lax.rem(chip + off, chips), r + turned * (1 - 2 * r)

    def at(ref, shard, h):
        return ref.at[shard, pl.ds(pl.multiple_of(h * half, half), half)]

    def of_core(ref, i, k):
        c, h = place(i)
        return at(ref, c * CORES + k, h)

    own = (dy, x)
    gathered = (dy_all, x_all)

    def own_half(w, h):
        return own[w].at[pl.ds(h * half, half)]

    def remote(src, dst, s, r, dev):
        return pltpu.make_async_remote_copy(
            src_ref=src, dst_ref=dst, send_sem=s, recv_sem=r, device_id={"tp": dev}, device_id_type=MESH
        )

    def ring_own(w, j):
        h = {2: 0, 3: 1, 4: 1, 5: 0}[j]
        return remote(own_half(w, h), at(gathered[w], me, h), ring_s.at[w, j], ring_r.at[w, j], right if j % 2 == 0 else left)

    def ring_relay(w, j):
        ref = of_core(gathered[w], j - 4, core)
        return remote(ref, ref, ring_s.at[w, j], ring_r.at[w, j], right if j % 2 == 0 else left)

    def ring_send(w, j):
        return ring_own(w, j) if j < 6 else ring_relay(w, j)

    def ring_got(w, j):
        ref = of_core(gathered[w], j, core)
        return remote(ref, ref, ring_s.at[w, j], ring_r.at[w, j], right)

    def to_partner(w, j):
        src = own_half(w, j) if j < 2 else of_core(gathered[w], j, core)
        return remote(src, of_core(gathered[w], j, core), pair_s.at[w, j], pair_r.at[w, j], partner)

    def from_partner(w, j):
        ref = of_core(gathered[w], j, 1 - core)
        return remote(ref, ref, pair_s.at[w, j], pair_r.at[w, j], partner)

    def service(w, j):
        ring_got(w, j).wait_recv()
        if j < 4:
            ring_relay(w, j + 4).start()
        to_partner(w, j).start()

    def load(src, dst, sem):
        c = pltpu.make_async_copy(src, dst, sem)
        c.start()
        return c

    def start_rows(w, j):
        from_partner(w, j).wait_recv()
        slot = j % 2
        load(of_core(gathered[w], j, 1 - core), rows_buf.at[slot, pl.ds(0, half)], ld_sem.at[slot, 0])
        c, h = place(j)

        @pl.when(j < 2)
        def _():
            src = own[w].at[pl.ds(pl.multiple_of(h * half, half), half)]
            load(src, rows_buf.at[slot, pl.ds(half, half)], ld_sem.at[slot, 1])

        @pl.when(j >= 2)
        def _():
            load(of_core(gathered[w], j, core), rows_buf.at[slot, pl.ds(half, half)], ld_sem.at[slot, 1])

    def rows_of(w, j):
        @pl.when(j % 2 == 0)
        def _():
            start_rows(w, j)
            start_rows(w, j + 1)

        slot = j % 2
        for b in range(2):
            ref = rows_buf.at[slot, pl.ds(b * half, half)]
            pltpu.make_async_copy(ref, ref, ld_sem.at[slot, b]).wait()
        return rows_buf.at[slot]

    def pre_load(j, b):
        c, h = place(j)
        where = (1 - core) if b == 0 else core
        start = pl.multiple_of((c * CORES + where) * size + h * half, half)
        return pltpu.make_async_copy(
            pre.at[pl.ds(start, half)], pre_buf.at[j % 2, pl.ds(b * half, half)], pre_sem.at[j % 2, b]
        )

    def pair_sum(j):
        return remote(st_pair.at[pl.ds(pl.multiple_of(j % 2 * half, half), half)], pair_buf.at[j % 2], rsp_s.at[j], rsp_r.at[j], partner)

    def ring_sum(j):
        dev = lax.rem(me + n - CORES + 2 * CORES * (j % 2), n)
        return remote(st_ring.at[j - 4], ring_buf.at[j - 4], rsg_s.at[j - 4], rsg_r.at[j - 4], dev)

    def chain_send(b, q):
        ref = (b, pl.ds(q * piece, piece))
        return remote(st_ring.at[ref], chain_buf.at[ref], ch_s.at[b, q], ch_r.at[b, q], left if b == 0 else right)

    barrier = pltpu.get_barrier_semaphore()
    for dev in (left, right, partner):
        pl.semaphore_signal(barrier, inc=1, device_id={"tp": dev}, device_id_type=MESH)
    pl.semaphore_wait(barrier, 3)

    for j in (2, 3, 4, 5):
        ring_own(DY, j).start()
    for j in (0, 1):
        to_partner(DY, j).start()
    for b in range(2):
        pre_load(0, b).start()
    load(w_down, wd, w_sem.at[0])
    load(w_in, wi, w_sem.at[1])

    @pl.loop(0, ff, step=64)
    def _(r):
        acc_down[pl.ds(pl.multiple_of(r, 64), 64)] = jnp.zeros((64, d), F32)

    @pl.loop(0, d, step=128)
    def _(r):
        acc_in[pl.ds(pl.multiple_of(r, 128), 128)] = jnp.zeros((128, ff), F32)

    pltpu.make_async_copy(w_down, wd, w_sem.at[0]).wait()
    pltpu.make_async_copy(w_in, wi, w_sem.at[1]).wait()

    tile = 256

    @pl.loop(0, PAIRS)
    def _(i):
        slot = i % 2

        @pl.when(i == 2)
        def _():
            service(DY, 2)
            service(DY, 3)
            ring_own(X, 2).start()
            ring_own(X, 3).start()
            to_partner(X, 0).start()
            to_partner(X, 1).start()

        @pl.when(i == 4)
        def _():
            service(DY, 4)
            service(DY, 5)
            ring_own(X, 4).start()
            ring_own(X, 5).start()

        @pl.when(i == 6)
        def _():
            service(DY, 6)
            service(DY, 7)

        @pl.when(i < PAIRS - 1)
        def _():
            for b in range(2):
                pre_load(i + 1, b).start()

        rows = rows_of(DY, i)
        for b in range(2):
            pre_load(i, b).wait()

        @pl.loop(0, ff, step=tile)
        def _(f):
            fs = pl.ds(pl.multiple_of(f, tile), tile)
            dh = lax.dot_general(rows[...], wd[fs, :], NT, preferred_element_type=F32)
            h, slope = gelu_and_slope(pre_buf[slot, :, fs].astype(F32))
            dpre[i, :, fs] = (dh * slope).astype(BF16)
            hid[:, fs] = h.astype(BF16)

        @pl.when(i >= 2)
        def _():
            pair_sum(i - 2).wait_send()

        @pl.loop(0, d, step=2 * tile)
        def _(c):
            cs = pl.ds(pl.multiple_of(c, 2 * tile), 2 * tile)
            o = lax.dot_general(dpre[i, 0:half, :], wi[cs, :], NT, preferred_element_type=F32)
            st_pair[pl.ds(pl.multiple_of(slot * half, half), half), cs] = o.astype(BF16)

        pair_sum(i).start()

        @pl.loop(0, ff, step=tile)
        def _(f):
            fs = pl.ds(pl.multiple_of(f, tile), tile)

            for c in range(0, d, 2 * tile):
                acc_down[fs, c : c + 2 * tile] += lax.dot_general(
                    hid[:, fs], rows[:, c : c + 2 * tile], TN, preferred_element_type=F32
                )

        pair_sum(i).wait_recv()

        def mine(c):
            cs = pl.ds(pl.multiple_of(c, 2 * tile), 2 * tile)
            o = lax.dot_general(dpre[i, half : 2 * half, :], wi[cs, :], NT, preferred_element_type=F32)
            return cs, o + pair_buf[slot, :, cs].astype(F32)

        @pl.when(i < 4)
        def _():
            @pl.loop(0, d, step=2 * tile)
            def _(c):
                cs, o = mine(c)
                stash[i, :, cs] = o

        @pl.when(i >= 4)
        def _():
            @pl.loop(0, d, step=2 * tile)
            def _(c):
                cs, o = mine(c)
                st_ring[i - 4, :, cs] = o.astype(BF16)

            ring_sum(i).start()

    service(X, 2)
    service(X, 3)

    for b in range(2):
        pair_sum(PAIRS - 2 + b).wait_send()

    @pl.loop(0, ff, step=32)
    def _(r):
        rs = pl.ds(pl.multiple_of(r, 32), 32)
        dw_down[rs] = acc_down[rs].astype(BF16)

    def chain(b):
        ring_sum(6 + b).wait_recv()
        ring_sum(4 + b).wait_send()

        @pl.loop(0, half, step=32)
        def _(r):
            rs = pl.ds(pl.multiple_of(r, 32), 32)
            st_ring[b, rs] = (stash[2 + b, rs] + ring_buf[2 + b, rs].astype(F32)).astype(BF16)

        for q in range(PIECES):
            chain_send(b, q).start()

    def direct(b):
        ring_sum(4 + b).wait_recv()

        @pl.loop(0, half, step=32)
        def _(r):
            rs = pl.ds(pl.multiple_of(r, 32), 32)
            stash[1 - b, rs] += ring_buf[b, rs].astype(F32)

    @pl.loop(0, PAIRS)
    def _(i):
        @pl.when(i == 4)
        def _():
            direct(0)
            direct(1)
            chain(0)
            chain(1)
            service(X, 4)
            service(X, 5)

        @pl.when(i == 6)
        def _():
            service(X, 6)
            service(X, 7)

        rows = rows_of(X, i)

        @pl.loop(0, d, step=tile)
        def _(c):
            cs = pl.ds(pl.multiple_of(c, tile), tile)

            for f in range(0, ff, 2 * tile):
                acc_in[cs, f : f + 2 * tile] += lax.dot_general(
                    rows[:, cs], dpre[i, :, f : f + 2 * tile], TN, preferred_element_type=F32
                )

    @pl.loop(0, d, step=64)
    def _(r):
        rs = pl.ds(pl.multiple_of(r, 64), 64)
        dw_in[rs] = acc_in[rs].astype(BF16)

    for w in (DY, X):
        for j in range(2, PAIRS):
            ring_send(w, j).wait_send()
        for j in range(PAIRS):
            to_partner(w, j).wait_send()
    for j in (6, 7):
        ring_sum(j).wait_send()

    for q in range(PIECES):
        for b in range(2):
            chain_send(b, q).wait_recv()
            rs = pl.ds(q * piece, piece)
            dx[pl.ds(b * half + q * piece, piece)] = (stash[b, rs] + chain_buf[b, rs].astype(F32)).astype(BF16)

    for b in range(2):
        for q in range(PIECES):
            chain_send(b, q).wait_send()


def results(*refs):
    count = len(refs) // 2
    ins, outs, sem = refs[:count], refs[count : 2 * count], refs[-1]
    copies = []
    for a, b in zip(ins, outs):
        rows = a.shape[0] // 2
        for i in range(2):
            rs = pl.ds(i * rows, rows)
            copies.append(pltpu.make_async_copy(a.at[rs], b.at[rs], sem.at[len(copies)]))
    for c in copies:
        c.start()
    for c in copies:
        c.wait()


def solution(mesh):
    n = mesh.shape["tp"]

    def step(x, dy, pre, w_in, w_down):
        (size, d), ff = x.shape, pre.shape[1]
        half = size // 2
        any_space = pl.BlockSpec(memory_space=pl.ANY)
        shapes = ((size, d), (d, ff), (ff, d))
        dma = pltpu.SemaphoreType.DMA
        outs = pl.pallas_call(
            functools.partial(kernel, n),
            out_shape=[pltpu.VMEM(s, BF16) for s in shapes]
            + [
                jax.ShapeDtypeStruct(s, BF16)
                for s in ((n, size, d), (n, size, d))
            ],
            in_specs=[any_space] * 5,
            out_specs=[pl.BlockSpec(memory_space=pltpu.VMEM)] * 3 + [any_space] * 2,
            scratch_shapes=[
                pltpu.VMEM((d, ff), F32),
                pltpu.VMEM((ff, d), F32),
                pltpu.VMEM((PAIRS, size, ff), BF16),
                pltpu.VMEM((4, half, d), F32),
                pltpu.VMEM((4, half, d), BF16),
                pltpu.VMEM((2, size, d), BF16),
                pltpu.VMEM((2, size, ff), BF16),
                pltpu.VMEM((size, ff), BF16),
                pltpu.VMEM((2, half, d), BF16),
                pltpu.VMEM((4, half, d), BF16),
                pltpu.VMEM((2, half, d), BF16),
                dma((2, PAIRS)), dma((2, PAIRS)), dma((2, PAIRS)), dma((2, PAIRS)),
                dma((PAIRS,)), dma((PAIRS,)), dma((4,)), dma((4,)), dma((2, PIECES)), dma((2, PIECES)),
                dma((2,)), dma((2, 2)), dma((2, 2)),
            ],
            compiler_params=pltpu.CompilerParams(collective_id=0, has_side_effects=True, vmem_limit_bytes=VMEM_LIMIT),
            name="mlp_backward",
        )(x, dy, pre, w_in, w_down)
        return tuple(
            pl.pallas_call(
                results,
                out_shape=[jax.ShapeDtypeStruct(s, BF16) for s in shapes],
                in_specs=[pl.BlockSpec(memory_space=pltpu.VMEM)] * 3,
                out_specs=[any_space] * 3,
                scratch_shapes=[dma((6,))],
                compiler_params=pltpu.CompilerParams(vmem_limit_bytes=2**20),
                name="results",
            )(*(pltpu.with_memory_space_constraint(o, pltpu.VMEM) for o in outs[:3]))
        )

    rows = P(("dp", "tp"), None)
    return jax.shard_map(
        step,
        mesh=mesh,
        in_specs=(rows, rows, P("dp", "tp"), P(None, "tp"), P("tp", None)),
        out_specs=(rows, P("dp", "tp"), rows),
        check_vma=False,
    )
```

```python
import functools

import jax
import jax.numpy as jnp
from jax import lax
from jax.experimental import pallas as pl
from jax.experimental.pallas import tpu as pltpu
from jax.sharding import PartitionSpec as P

MESH = pl.DeviceIdType.MESH
F32, BF16 = jnp.float32, jnp.bfloat16
CORES = 2
PAIRS = 8
LAST = 32
NT = (((1,), (1,)), ((), ()))
TN = (((0,), (0,)), ((), ()))
DY, X = 0, 1
VMEM_LIMIT = 53 * 2**20


def gelu_and_slope(p):
    c = 0.7978845608028654
    sq = p * p
    t = jnp.tanh(c * (p + 0.044715 * (sq * p)))
    cdf = 0.5 * (1.0 + t)
    slope = cdf + (0.5 * p) * (1.0 - t * t) * (c * (1.0 + 0.134145 * sq))
    return p * cdf, slope


def kernel(
    n, x, dy, pre, w_in, w_down,
    dx, dw_in, dw_down, x_all, dy_all,
    acc_in, acc_down, dpre, stash, st_ring, rows_buf, pre_buf, hid, pair_buf, ring_buf, chain_buf,
    ring_s, ring_r, pair_s, pair_r, rsp_s, rsp_r, sum_s, rsg_r, ch_r, w_sem, pre_sem, ld_sem,
):
    wi, wd, st_pair = dw_in, dw_down, dx
    me = lax.axis_index("tp")
    core = lax.rem(me, CORES)
    chip = me // CORES
    chips = n // CORES
    right = lax.rem(me + CORES, n)
    left = lax.rem(me + n - CORES, n)
    partner = me + 1 - 2 * core
    size, ff = x.shape[0], pre.shape[1]
    d = x.shape[1]
    half = size // 2

    def place(i):
        q, r = i // 2, i % 2
        odd = ((q + 1) // 2) % 2
        off = odd * (chips - 1 + 2 * r) + 2 * (q // 3)
        turned = (q // 2) * (1 - q // 3)
        return lax.rem(chip + off, chips), r + turned * (1 - 2 * r)

    def at(ref, shard, h):
        return ref.at[shard, pl.ds(pl.multiple_of(h * half, half), half)]

    def of_core(ref, i, k):
        c, h = place(i)
        return at(ref, c * CORES + k, h)

    own = (dy, x)
    gathered = (dy_all, x_all)

    def own_half(w, h):
        return own[w].at[pl.ds(h * half, half)]

    def remote(src, dst, s, r, dev):
        return pltpu.make_async_remote_copy(
            src_ref=src, dst_ref=dst, send_sem=s, recv_sem=r, device_id={"tp": dev}, device_id_type=MESH
        )

    def ring_own(w, j):
        h = {2: 0, 3: 1, 4: 1, 5: 0}[j]
        return remote(own_half(w, h), at(gathered[w], me, h), ring_s.at[0], ring_r.at[w, j - 2], right if j % 2 == 0 else left)

    def ring_relay(w, j):
        ref = of_core(gathered[w], j - 4, core)
        return remote(ref, ref, ring_s.at[0], ring_r.at[w, j - 2], right if j % 2 == 0 else left)

    def ring_send(w, j):
        return ring_own(w, j) if j < 6 else ring_relay(w, j)

    def ring_got(w, j):
        ref = of_core(gathered[w], j, core)
        return remote(ref, ref, ring_s.at[0], ring_r.at[w, j - 2], right)

    def to_partner(w, j):
        src = own_half(w, j) if j < 2 else of_core(gathered[w], j, core)
        return remote(src, of_core(gathered[w], j, core), pair_s.at[0], pair_r.at[j], partner)

    def from_partner(w, j):
        ref = of_core(gathered[w], j, 1 - core)
        return remote(ref, ref, pair_s.at[0], pair_r.at[j], partner)

    def service(w, j):
        ring_got(w, j).wait_recv()
        if j < 4:
            ring_relay(w, j + 4).start()
        to_partner(w, j).start()

    def load(src, dst, sem):
        c = pltpu.make_async_copy(src, dst, sem)
        c.start()
        return c

    def start_rows(w, j):
        from_partner(w, j).wait_recv()
        slot = j % 2
        load(of_core(gathered[w], j, 1 - core), rows_buf.at[slot, pl.ds(0, half)], ld_sem.at[slot])
        c, h = place(j)

        @pl.when(j < 2)
        def _():
            src = own[w].at[pl.ds(pl.multiple_of(h * half, half), half)]
            load(src, rows_buf.at[slot, pl.ds(half, half)], ld_sem.at[slot])

        @pl.when(j >= 2)
        def _():
            load(of_core(gathered[w], j, core), rows_buf.at[slot, pl.ds(half, half)], ld_sem.at[slot])

    def rows_of(j):
        slot = j % 2
        pltpu.make_async_copy(rows_buf.at[slot], rows_buf.at[slot], ld_sem.at[slot]).wait()
        return rows_buf.at[slot]

    def pre_load(j, b):
        c, h = place(j)
        where = (1 - core) if b == 0 else core
        start = pl.multiple_of((c * CORES + where) * size + h * half, half)
        return pltpu.make_async_copy(
            pre.at[pl.ds(start, half)], pre_buf.at[j % 2, pl.ds(b * half, half)], pre_sem.at[j % 2]
        )

    def pair_sum(j):
        return remote(st_pair.at[pl.ds(pl.multiple_of(j % 2 * half, half), half)], pair_buf.at[j % 2], rsp_s.at[j % 2], rsp_r.at[j % 2], partner)

    def ring_sum(j):
        dev = lax.rem(me + n - CORES + 2 * CORES * (j % 2), n)
        return remote(st_ring.at[j - 4], ring_buf.at[j - 4], sum_s.at[j - 4 - (j - 4) // 3], rsg_r.at[j - 4], dev)

    pieces = ((0, half - LAST), (half - LAST, LAST))

    def chain_send(b, q):
        ref = (b, pl.ds(*pieces[q]))
        return remote(st_ring.at[ref], chain_buf.at[ref], sum_s.at[2], ch_r.at[b, q], left if b == 0 else right)

    barrier = pltpu.get_barrier_semaphore()
    for dev in (left, right, partner):
        pl.semaphore_signal(barrier, inc=1, device_id={"tp": dev}, device_id_type=MESH)
    pl.semaphore_wait(barrier, 3)

    for j in (2, 3, 4, 5):
        ring_own(DY, j).start()
    for j in (0, 1):
        to_partner(DY, j).start()
    for b in range(2):
        pre_load(0, b).start()
    load(w_down, wd, w_sem.at[0])
    load(w_in, wi, w_sem.at[1])

    @pl.loop(0, ff, step=64)
    def _(r):
        acc_down[pl.ds(pl.multiple_of(r, 64), 64)] = jnp.zeros((64, d), F32)

    @pl.loop(0, d, step=128)
    def _(r):
        acc_in[pl.ds(pl.multiple_of(r, 128), 128)] = jnp.zeros((128, ff), F32)

    start_rows(DY, 0)
    pltpu.make_async_copy(w_down, wd, w_sem.at[0]).wait()
    pltpu.make_async_copy(w_in, wi, w_sem.at[1]).wait()

    tile = 256

    @pl.loop(0, PAIRS)
    def _(i):
        slot = i % 2

        @pl.when(i == 1)
        def _():
            service(DY, 2)
            service(DY, 3)
            ring_own(X, 2).start()
            ring_own(X, 3).start()
            to_partner(X, 0).start()
            to_partner(X, 1).start()

        @pl.when(i == 3)
        def _():
            service(DY, 4)
            service(DY, 5)
            ring_own(X, 4).start()
            ring_own(X, 5).start()

        @pl.when(i == 5)
        def _():
            service(DY, 6)
            service(DY, 7)

        @pl.when(i < PAIRS - 1)
        def _():
            start_rows(DY, i + 1)
            for b in range(2):
                pre_load(i + 1, b).start()

        rows = rows_of(i)
        pltpu.make_async_copy(pre_buf.at[slot], pre_buf.at[slot], pre_sem.at[slot]).wait()

        @pl.loop(0, ff, step=tile)
        def _(f):
            fs = pl.ds(pl.multiple_of(f, tile), tile)
            dh = lax.dot_general(rows[...], wd[fs, :], NT, preferred_element_type=F32)
            h, slope = gelu_and_slope(pre_buf[slot, :, fs].astype(F32))
            dpre[i, :, fs] = (dh * slope).astype(BF16)
            hid[:, fs] = h.astype(BF16)

        @pl.when(i >= 2)
        def _():
            pair_sum(i - 2).wait_send()

        @pl.loop(0, d, step=2 * tile)
        def _(c):
            cs = pl.ds(pl.multiple_of(c, 2 * tile), 2 * tile)
            o = lax.dot_general(dpre[i, 0:half, :], wi[cs, :], NT, preferred_element_type=F32)
            st_pair[pl.ds(pl.multiple_of(slot * half, half), half), cs] = o.astype(BF16)

        pair_sum(i).start()

        @pl.loop(0, ff, step=tile)
        def _(f):
            fs = pl.ds(pl.multiple_of(f, tile), tile)

            for c in range(0, d, 2 * tile):
                acc_down[fs, c : c + 2 * tile] += lax.dot_general(
                    hid[:, fs], rows[:, c : c + 2 * tile], TN, preferred_element_type=F32
                )

        pair_sum(i).wait_recv()

        def mine(c):
            cs = pl.ds(pl.multiple_of(c, 2 * tile), 2 * tile)
            o = lax.dot_general(dpre[i, half : 2 * half, :], wi[cs, :], NT, preferred_element_type=F32)
            return cs, o + pair_buf[slot, :, cs].astype(F32)

        @pl.when(i < 4)
        def _():
            @pl.loop(0, d, step=2 * tile)
            def _(c):
                cs, o = mine(c)
                stash[i, :, cs] = o

        @pl.when(i >= 4)
        def _():
            @pl.loop(0, d, step=2 * tile)
            def _(c):
                cs, o = mine(c)
                st_ring[i - 4, :, cs] = o.astype(BF16)

            ring_sum(i).start()

    service(X, 2)
    service(X, 3)
    start_rows(X, 0)
    for b in range(2):
        pair_sum(PAIRS - 2 + b).wait_send()

    @pl.loop(0, ff, step=32)
    def _(r):
        rs = pl.ds(pl.multiple_of(r, 32), 32)
        dw_down[rs] = acc_down[rs].astype(BF16)

    def chain(b):
        ring_sum(6 + b).wait_recv()
        ring_sum(4 + b).wait_send()

        @pl.loop(0, half, step=32)
        def _(r):
            rs = pl.ds(pl.multiple_of(r, 32), 32)
            st_ring[b, rs] = (stash[2 + b, rs] + ring_buf[2 + b, rs].astype(F32)).astype(BF16)

        for q in range(len(pieces)):
            chain_send(b, q).start()

    def direct(b):
        ring_sum(4 + b).wait_recv()

        @pl.loop(0, half, step=32)
        def _(r):
            rs = pl.ds(pl.multiple_of(r, 32), 32)
            stash[1 - b, rs] += ring_buf[b, rs].astype(F32)

    @pl.loop(0, PAIRS)
    def _(i):
        @pl.when(i == 3)
        def _():
            service(X, 4)
            service(X, 5)

        @pl.when(i == PAIRS - 2)
        def _():
            direct(0)
            direct(1)
            chain(0)
            chain(1)
            service(X, 6)
            service(X, 7)
            start_rows(X, i)
            start_rows(X, i + 1)

        @pl.when(i < PAIRS - 3)
        def _():
            start_rows(X, i + 1)

        rows = rows_of(i)

        @pl.loop(0, d, step=tile)
        def _(c):
            cs = pl.ds(pl.multiple_of(c, tile), tile)

            for f in range(0, ff, 2 * tile):
                acc_in[cs, f : f + 2 * tile] += lax.dot_general(
                    rows[:, cs], dpre[i, :, f : f + 2 * tile], TN, preferred_element_type=F32
                )

    @pl.loop(0, d, step=64)
    def _(r):
        rs = pl.ds(pl.multiple_of(r, 64), 64)
        dw_in[rs] = acc_in[rs].astype(BF16)

    ring_sent = x_all.at[pl.ds(0, PAIRS - 2)]
    remote(ring_sent, ring_sent, ring_s.at[0], ring_r.at[0, 0], right).wait_send()
    remote(x_all, x_all, pair_s.at[0], pair_r.at[0], partner).wait_send()

    for q in range(len(pieces)):
        for b in range(2):
            chain_send(b, q).wait_recv()

            @pl.loop(0, pieces[q][1], step=LAST)
            def _(r):
                rs = pl.ds(pl.multiple_of(pieces[q][0] + r, LAST), LAST)
                to = pl.ds(pl.multiple_of(b * half + pieces[q][0] + r, LAST), LAST)
                dx[to] = (stash[b, rs] + chain_buf[b, rs].astype(F32)).astype(BF16)

    remote(st_ring, ring_buf, sum_s.at[2], rsg_r.at[0], left).wait_send()


def results(*refs):
    count = len(refs) // 2
    ins, outs, sem = refs[:count], refs[count : 2 * count], refs[-1]
    for i, (a, b) in enumerate(zip(ins, outs)):
        rows = a.shape[0] // 2
        for start in (0, rows):
            rs = pl.ds(start, rows)
            pltpu.make_async_copy(a.at[rs], b.at[rs], sem.at[i]).start()
    for i, (a, b) in enumerate(zip(ins, outs)):
        pltpu.make_async_copy(a, b, sem.at[i]).wait()


def solution(mesh):
    n = mesh.shape["tp"]

    def step(x, dy, pre, w_in, w_down):
        (size, d), ff = x.shape, pre.shape[1]
        half = size // 2
        any_space = pl.BlockSpec(memory_space=pl.ANY)
        shapes = ((size, d), (d, ff), (ff, d))
        dma = pltpu.SemaphoreType.DMA
        outs = pl.pallas_call(
            functools.partial(kernel, n),
            out_shape=[pltpu.VMEM(s, BF16) for s in shapes]
            + [
                jax.ShapeDtypeStruct(s, BF16)
                for s in ((n, size, d), (n, size, d))
            ],
            in_specs=[any_space] * 5,
            out_specs=[pl.BlockSpec(memory_space=pltpu.VMEM)] * 3 + [any_space] * 2,
            scratch_shapes=[
                pltpu.VMEM((d, ff), F32),
                pltpu.VMEM((ff, d), F32),
                pltpu.VMEM((PAIRS, size, ff), BF16),
                pltpu.VMEM((4, half, d), F32),
                pltpu.VMEM((4, half, d), BF16),
                pltpu.VMEM((2, size, d), BF16),
                pltpu.VMEM((2, size, ff), BF16),
                pltpu.VMEM((size, ff), BF16),
                pltpu.VMEM((2, half, d), BF16),
                pltpu.VMEM((4, half, d), BF16),
                pltpu.VMEM((2, half, d), BF16),
                dma((1,)), dma((2, PAIRS - 2)), dma((1,)), dma((PAIRS,)), dma((2,)), dma((2,)), dma((3,)), dma((4,)),
                dma((2, 2)), dma((2,)), dma((2,)), dma((2,)),
            ],
            compiler_params=pltpu.CompilerParams(collective_id=0, has_side_effects=True, vmem_limit_bytes=VMEM_LIMIT),
            name="mlp_backward",
        )(x, dy, pre, w_in, w_down)
        return tuple(
            pl.pallas_call(
                results,
                out_shape=[jax.ShapeDtypeStruct(s, BF16) for s in shapes],
                in_specs=[pl.BlockSpec(memory_space=pltpu.VMEM)] * 3,
                out_specs=[any_space] * 3,
                scratch_shapes=[dma((3,))],
                compiler_params=pltpu.CompilerParams(vmem_limit_bytes=2**20),
                name="results",
            )(*(pltpu.with_memory_space_constraint(o, pltpu.VMEM) for o in outs[:3]))
        )

    rows = P(("dp", "tp"), None)
    return jax.shard_map(
        step,
        mesh=mesh,
        in_specs=(rows, rows, P("dp", "tp"), P(None, "tp"), P("tp", None)),
        out_specs=(rows, P("dp", "tp"), rows),
        check_vma=False,
    )
```

```python
import functools

import jax
import jax.numpy as jnp
from jax import lax
from jax.experimental import pallas as pl
from jax.experimental.pallas import tpu as pltpu
from jax.sharding import PartitionSpec as P

MESH = pl.DeviceIdType.MESH
F32, BF16 = jnp.float32, jnp.bfloat16
CORES = 2
PAIRS = 8
LAST = 32
NT = (((1,), (1,)), ((), ()))
TN = (((0,), (0,)), ((), ()))
DY, X = 0, 1
VMEM_LIMIT = 53 * 2**20


def gelu_and_slope(p):
    c = 0.7978845608028654
    sq = p * p
    t = jnp.tanh(c * (p + 0.044715 * (sq * p)))
    cdf = 0.5 * (1.0 + t)
    slope = cdf + (0.5 * p) * (1.0 - t * t) * (c * (1.0 + 0.134145 * sq))
    return p * cdf, slope


def kernel(
    n, x, dy, pre, w_in, w_down,
    dx, dw_in, dw_down, x_all, dy_all,
    acc_in, acc_down, dpre, stash, st_ring, rows_buf, pre_buf, hid, pair_buf, ring_buf, chain_buf,
    ring_s, ring_r, pair_s, pair_r, rsp_s, rsp_r, sum_s, sum_r, ch_r, w_sem, pre_sem, ld_sem,
):
    wi, wd, st_pair = dw_in, dw_down, dx
    me = lax.axis_index("tp")
    core = lax.rem(me, CORES)
    chip = me // CORES
    chips = n // CORES
    right = lax.rem(me + CORES, n)
    left = lax.rem(me + n - CORES, n)
    partner = me + 1 - 2 * core
    size, ff = x.shape[0], pre.shape[1]
    d = x.shape[1]
    half = size // 2

    def place(i):
        q, r = i // 2, i % 2
        odd = ((q + 1) // 2) % 2
        off = odd * (chips - 1 + 2 * r) + 2 * (q // 3)
        turned = (q // 2) * (1 - q // 3)
        return lax.rem(chip + off, chips), r + turned * (1 - 2 * r)

    def at(ref, shard, h):
        return ref.at[shard, pl.ds(pl.multiple_of(h * half, half), half)]

    def of_core(ref, i, k):
        c, h = place(i)
        return at(ref, c * CORES + k, h)

    own = (dy, x)
    gathered = (dy_all, x_all)

    def own_half(w, h):
        return own[w].at[pl.ds(h * half, half)]

    def remote(src, dst, s, r, dev):
        return pltpu.make_async_remote_copy(
            src_ref=src, dst_ref=dst, send_sem=s, recv_sem=r, device_id={"tp": dev}, device_id_type=MESH
        )

    def ring_own(w, j):
        h = {2: 0, 3: 1, 4: 1, 5: 0}[j]
        return remote(own_half(w, h), at(gathered[w], me, h), ring_s.at[0], ring_r.at[w, j // 2 - 1], right if j % 2 == 0 else left)

    def ring_relay(w, j):
        ref = of_core(gathered[w], j - 4, core)
        return remote(ref, ref, ring_s.at[0], ring_r.at[w, j // 2 - 1], right if j % 2 == 0 else left)

    def ring_send(w, j):
        return ring_own(w, j) if j < 6 else ring_relay(w, j)

    def to_partner(w, j):
        src = own_half(w, j) if j < 2 else of_core(gathered[w], j, core)
        return remote(src, of_core(gathered[w], j, core), pair_s.at[0], pair_r.at[j // 2], partner)

    def service(w, j):
        both = gathered[w].at[0]
        remote(both, both, ring_s.at[0], ring_r.at[w, j // 2 - 1], right).wait_recv()
        for q in (j, j + 1):
            if q < 4:
                ring_relay(w, q + 4).start()
            to_partner(w, q).start()

    def load(src, dst, sem):
        c = pltpu.make_async_copy(src, dst, sem)
        c.start()
        return c

    def start_rows(w, j):
        @pl.when(j % 2 == 0)
        def _():
            both = gathered[w].at[0]
            remote(both, both, pair_s.at[0], pair_r.at[j // 2], partner).wait_recv()

        slot = j % 2
        load(of_core(gathered[w], j, 1 - core), rows_buf.at[slot, pl.ds(0, half)], ld_sem.at[slot])
        c, h = place(j)

        @pl.when(j < 2)
        def _():
            src = own[w].at[pl.ds(pl.multiple_of(h * half, half), half)]
            load(src, rows_buf.at[slot, pl.ds(half, half)], ld_sem.at[slot])

        @pl.when(j >= 2)
        def _():
            load(of_core(gathered[w], j, core), rows_buf.at[slot, pl.ds(half, half)], ld_sem.at[slot])

    def rows_of(j):
        slot = j % 2
        pltpu.make_async_copy(rows_buf.at[slot], rows_buf.at[slot], ld_sem.at[slot]).wait()
        return rows_buf.at[slot]

    def pre_load(j, b):
        c, h = place(j)
        where = (1 - core) if b == 0 else core
        start = pl.multiple_of((c * CORES + where) * size + h * half, half)
        return pltpu.make_async_copy(
            pre.at[pl.ds(start, half)], pre_buf.at[j % 2, pl.ds(b * half, half)], pre_sem.at[j % 2]
        )

    def pair_sum(j):
        return remote(st_pair.at[pl.ds(pl.multiple_of(j % 2 * half, half), half)], pair_buf.at[j % 2], rsp_s.at[j % 2], rsp_r.at[j % 2], partner)

    def ring_sum(j):
        dev = lax.rem(me + n - CORES + 2 * CORES * (j % 2), n)
        return remote(st_ring.at[j - 4], ring_buf.at[j - 4], sum_s.at[j // 2 - 2], sum_r.at[j // 2 - 2], dev)

    pieces = ((0, half - LAST), (half - LAST, LAST))

    def chain_send(b, q):
        ref = (b, pl.ds(*pieces[q]))
        return remote(st_ring.at[ref], chain_buf.at[ref], sum_s.at[1], ch_r.at[q], left if b == 0 else right)

    barrier = pltpu.get_barrier_semaphore()
    for dev in (left, right, partner):
        pl.semaphore_signal(barrier, inc=1, device_id={"tp": dev}, device_id_type=MESH)
    pl.semaphore_wait(barrier, 3)

    for j in (2, 3, 4, 5):
        ring_own(DY, j).start()
    for j in (0, 1):
        to_partner(DY, j).start()
    for b in range(2):
        pre_load(0, b).start()
    load(w_down, wd, w_sem.at[0])
    load(w_in, wi, w_sem.at[1])

    @pl.loop(0, ff, step=64)
    def _(r):
        acc_down[pl.ds(pl.multiple_of(r, 64), 64)] = jnp.zeros((64, d), F32)

    @pl.loop(0, d, step=128)
    def _(r):
        acc_in[pl.ds(pl.multiple_of(r, 128), 128)] = jnp.zeros((128, ff), F32)

    start_rows(DY, 0)
    pltpu.make_async_copy(w_down, wd, w_sem.at[0]).wait()
    pltpu.make_async_copy(w_in, wi, w_sem.at[1]).wait()

    tile = 256

    @pl.loop(0, PAIRS)
    def _(i):
        slot = i % 2

        @pl.when(i == 1)
        def _():
            service(DY, 2)
            ring_own(X, 2).start()
            ring_own(X, 3).start()
            to_partner(X, 0).start()
            to_partner(X, 1).start()

        @pl.when(i == 3)
        def _():
            service(DY, 4)
            ring_own(X, 4).start()
            ring_own(X, 5).start()

        @pl.when(i == 5)
        def _():
            service(DY, 6)

        @pl.when(i < PAIRS - 1)
        def _():
            start_rows(DY, i + 1)
            for b in range(2):
                pre_load(i + 1, b).start()

        rows = rows_of(i)
        pltpu.make_async_copy(pre_buf.at[slot], pre_buf.at[slot], pre_sem.at[slot]).wait()

        @pl.loop(0, ff, step=tile)
        def _(f):
            fs = pl.ds(pl.multiple_of(f, tile), tile)
            dh = lax.dot_general(rows[...], wd[fs, :], NT, preferred_element_type=F32)
            h, slope = gelu_and_slope(pre_buf[slot, :, fs].astype(F32))
            dpre[i, :, fs] = (dh * slope).astype(BF16)
            hid[:, fs] = h.astype(BF16)

        @pl.when(i >= 2)
        def _():
            pair_sum(i - 2).wait_send()

        @pl.loop(0, d, step=2 * tile)
        def _(c):
            cs = pl.ds(pl.multiple_of(c, 2 * tile), 2 * tile)
            o = lax.dot_general(dpre[i, 0:half, :], wi[cs, :], NT, preferred_element_type=F32)
            st_pair[pl.ds(pl.multiple_of(slot * half, half), half), cs] = o.astype(BF16)

        pair_sum(i).start()

        @pl.loop(0, ff, step=tile)
        def _(f):
            fs = pl.ds(pl.multiple_of(f, tile), tile)

            for c in range(0, d, 2 * tile):
                acc_down[fs, c : c + 2 * tile] += lax.dot_general(
                    hid[:, fs], rows[:, c : c + 2 * tile], TN, preferred_element_type=F32
                )

        pair_sum(i).wait_recv()

        def mine(c):
            cs = pl.ds(pl.multiple_of(c, 2 * tile), 2 * tile)
            o = lax.dot_general(dpre[i, half : 2 * half, :], wi[cs, :], NT, preferred_element_type=F32)
            return cs, o + pair_buf[slot, :, cs].astype(F32)

        @pl.when(i < 4)
        def _():
            @pl.loop(0, d, step=2 * tile)
            def _(c):
                cs, o = mine(c)
                stash[i, :, cs] = o

        @pl.when(i >= 4)
        def _():
            @pl.loop(0, d, step=2 * tile)
            def _(c):
                cs, o = mine(c)
                st_ring[i - 4, :, cs] = o.astype(BF16)

            ring_sum(i).start()

    service(X, 2)
    start_rows(X, 0)
    for b in range(2):
        pair_sum(PAIRS - 2 + b).wait_send()

    @pl.loop(0, ff, step=32)
    def _(r):
        rs = pl.ds(pl.multiple_of(r, 32), 32)
        dw_down[rs] = acc_down[rs].astype(BF16)

    def hops(q):
        both = pl.ds(2 * q, 2)
        return remote(st_ring.at[both], ring_buf.at[both], sum_s.at[q], sum_r.at[q], right)

    def chain(b):
        @pl.loop(0, half, step=32)
        def _(r):
            rs = pl.ds(pl.multiple_of(r, 32), 32)
            st_ring[b, rs] = (stash[2 + b, rs] + ring_buf[2 + b, rs].astype(F32)).astype(BF16)

        for q in range(len(pieces)):
            chain_send(b, q).start()

    def direct(b):
        @pl.loop(0, half, step=32)
        def _(r):
            rs = pl.ds(pl.multiple_of(r, 32), 32)
            stash[1 - b, rs] += ring_buf[b, rs].astype(F32)

    @pl.loop(0, PAIRS)
    def _(i):
        @pl.when(i == 3)
        def _():
            service(X, 4)

        @pl.when(i == PAIRS - 2)
        def _():
            hops(0).wait()
            direct(0)
            direct(1)
            hops(1).wait_recv()
            chain(0)
            chain(1)
            service(X, 6)
            start_rows(X, i)
            start_rows(X, i + 1)

        @pl.when(i < PAIRS - 3)
        def _():
            start_rows(X, i + 1)

        rows = rows_of(i)

        @pl.loop(0, d, step=tile)
        def _(c):
            cs = pl.ds(pl.multiple_of(c, tile), tile)

            for f in range(0, ff, 2 * tile):
                acc_in[cs, f : f + 2 * tile] += lax.dot_general(
                    rows[:, cs], dpre[i, :, f : f + 2 * tile], TN, preferred_element_type=F32
                )

    @pl.loop(0, d, step=64)
    def _(r):
        rs = pl.ds(pl.multiple_of(r, 64), 64)
        dw_in[rs] = acc_in[rs].astype(BF16)

    ring_sent = x_all.at[pl.ds(0, PAIRS - 2)]
    remote(ring_sent, ring_sent, ring_s.at[0], ring_r.at[0, 0], right).wait_send()
    remote(x_all, x_all, pair_s.at[0], pair_r.at[0], partner).wait_send()

    for q in range(len(pieces)):
        both = chain_buf.at[:, pl.ds(*pieces[q])]
        remote(both, both, sum_s.at[1], ch_r.at[q], right).wait_recv()
        for b in range(2):

            @pl.loop(0, pieces[q][1], step=LAST)
            def _(r):
                rs = pl.ds(pl.multiple_of(pieces[q][0] + r, LAST), LAST)
                to = pl.ds(pl.multiple_of(b * half + pieces[q][0] + r, LAST), LAST)
                dx[to] = (stash[b, rs] + chain_buf[b, rs].astype(F32)).astype(BF16)

    remote(st_ring, ring_buf, sum_s.at[1], sum_r.at[1], left).wait_send()


def results(*refs):
    count = len(refs) // 2
    ins, outs, sem = refs[:count], refs[count : 2 * count], refs[-1]
    for i, (a, b) in enumerate(zip(ins, outs)):
        rows = a.shape[0] // 8
        for start in range(0, a.shape[0], rows):
            rs = pl.ds(start, rows)
            pltpu.make_async_copy(a.at[rs], b.at[rs], sem.at[i]).start()
    for i, (a, b) in enumerate(zip(ins, outs)):
        pltpu.make_async_copy(a, b, sem.at[i]).wait()


def solution(mesh):
    n = mesh.shape["tp"]

    def step(x, dy, pre, w_in, w_down):
        (size, d), ff = x.shape, pre.shape[1]
        half = size // 2
        any_space = pl.BlockSpec(memory_space=pl.ANY)
        shapes = ((size, d), (d, ff), (ff, d))
        dma = pltpu.SemaphoreType.DMA
        outs = pl.pallas_call(
            functools.partial(kernel, n),
            out_shape=[pltpu.VMEM(s, BF16) for s in shapes]
            + [
                jax.ShapeDtypeStruct(s, BF16)
                for s in ((n, size, d), (n, size, d))
            ],
            in_specs=[any_space] * 5,
            out_specs=[pl.BlockSpec(memory_space=pltpu.VMEM)] * 3 + [any_space] * 2,
            scratch_shapes=[
                pltpu.VMEM((d, ff), F32),
                pltpu.VMEM((ff, d), F32),
                pltpu.VMEM((PAIRS, size, ff), BF16),
                pltpu.VMEM((4, half, d), F32),
                pltpu.VMEM((4, half, d), BF16),
                pltpu.VMEM((2, size, d), BF16),
                pltpu.VMEM((2, size, ff), BF16),
                pltpu.VMEM((size, ff), BF16),
                pltpu.VMEM((2, half, d), BF16),
                pltpu.VMEM((4, half, d), BF16),
                pltpu.VMEM((2, half, d), BF16),
                dma((1,)), dma((2, 3)), dma((1,)), dma((PAIRS // 2,)), dma((2,)), dma((2,)), dma((2,)), dma((2,)),
                dma((2,)), dma((2,)), dma((2,)), dma((2,)),
            ],
            compiler_params=pltpu.CompilerParams(collective_id=0, has_side_effects=True, vmem_limit_bytes=VMEM_LIMIT),
            name="mlp_backward",
        )(x, dy, pre, w_in, w_down)
        return tuple(
            pl.pallas_call(
                results,
                out_shape=[jax.ShapeDtypeStruct(s, BF16) for s in shapes],
                in_specs=[pl.BlockSpec(memory_space=pltpu.VMEM)] * 3,
                out_specs=[any_space] * 3,
                scratch_shapes=[dma((3,))],
                compiler_params=pltpu.CompilerParams(vmem_limit_bytes=2**20),
                name="results",
            )(*(pltpu.with_memory_space_constraint(o, pltpu.VMEM) for o in outs[:3]))
        )

    rows = P(("dp", "tp"), None)
    return jax.shard_map(
        step,
        mesh=mesh,
        in_specs=(rows, rows, P("dp", "tp"), P(None, "tp"), P("tp", None)),
        out_specs=(rows, P("dp", "tp"), rows),
        check_vma=False,
    )
```

```python
import functools

import jax
import jax.numpy as jnp
from jax import lax
from jax.experimental import pallas as pl
from jax.experimental.pallas import tpu as pltpu
from jax.sharding import PartitionSpec as P

MESH = pl.DeviceIdType.MESH
F32, BF16 = jnp.float32, jnp.bfloat16
CORES = 2
PAIRS = 8
LAST = 16
ROWS = 8
NT = (((1,), (1,)), ((), ()))
TN = (((0,), (0,)), ((), ()))
DY, X = 0, 1
VMEM_LIMIT = 53 * 2**20


def gelu_and_slope(p):
    c = 0.7978845608028654
    sq = p * p
    t = jnp.tanh(c * (p + 0.044715 * (sq * p)))
    cdf = 0.5 * (1.0 + t)
    slope = cdf + (0.5 * p) * (1.0 - t * t) * (c * (1.0 + 0.134145 * sq))
    return p * cdf, slope


def kernel(
    n, x, dy, pre, w_in, w_down,
    dx, dw_in, dw_down, x_all, dy_all,
    acc_in, acc_down, dpre, stash, st_ring, rows_buf, pre_buf, hid, pair_buf, ring_buf, chain_buf,
    ring_s, ring_r, pair_s, pair_r, rsp_s, rsp_r, sum_s, sum_r, ch_r, w_sem, pre_sem, ld_sem,
):
    wi, wd, st_pair = dw_in, dw_down, dx
    me = lax.axis_index("tp")
    core = lax.rem(me, CORES)
    chip = me // CORES
    chips = n // CORES
    right = lax.rem(me + CORES, n)
    left = lax.rem(me + n - CORES, n)
    partner = me + 1 - 2 * core
    size, ff = x.shape[0], pre.shape[1]
    d = x.shape[1]
    half = size // 2

    def place(i):
        q, r = i // 2, i % 2
        odd = ((q + 1) // 2) % 2
        off = odd * (chips - 1 + 2 * r) + 2 * (q // 3)
        turned = (q // 2) * (1 - q // 3)
        return lax.rem(chip + off, chips), r + turned * (1 - 2 * r)

    def at(ref, shard, h):
        return ref.at[shard, pl.ds(pl.multiple_of(h * half, half), half)]

    def of_core(ref, i, k):
        c, h = place(i)
        return at(ref, c * CORES + k, h)

    own = (dy, x)
    gathered = (dy_all, x_all)

    def own_half(w, h):
        return own[w].at[pl.ds(h * half, half)]

    def remote(src, dst, s, r, dev):
        return pltpu.make_async_remote_copy(
            src_ref=src, dst_ref=dst, send_sem=s, recv_sem=r, device_id={"tp": dev}, device_id_type=MESH
        )

    def ring_own(w, j):
        h = {2: 0, 3: 1, 4: 1, 5: 0}[j]
        return remote(own_half(w, h), at(gathered[w], me, h), ring_s.at[0], ring_r.at[w, j // 2 - 1], right if j % 2 == 0 else left)

    def ring_relay(w, j):
        ref = of_core(gathered[w], j - 4, core)
        return remote(ref, ref, ring_s.at[0], ring_r.at[w, j // 2 - 1], right if j % 2 == 0 else left)

    def ring_send(w, j):
        return ring_own(w, j) if j < 6 else ring_relay(w, j)

    def to_partner(w, j):
        src = own_half(w, j) if j < 2 else of_core(gathered[w], j, core)
        return remote(src, of_core(gathered[w], j, core), pair_s.at[0], pair_r.at[j // 2], partner)

    def service(w, j):
        both = gathered[w].at[0]
        remote(both, both, ring_s.at[0], ring_r.at[w, j // 2 - 1], right).wait_recv()
        for q in (j, j + 1):
            if q < 4:
                ring_relay(w, q + 4).start()
            to_partner(w, q).start()

    def load(src, dst, sem):
        c = pltpu.make_async_copy(src, dst, sem)
        c.start()
        return c

    def start_rows(w, j):
        @pl.when(j % 2 == 0)
        def _():
            both = gathered[w].at[0]
            remote(both, both, pair_s.at[0], pair_r.at[j // 2], partner).wait_recv()

        slot = j % 2
        load(of_core(gathered[w], j, 1 - core), rows_buf.at[slot, pl.ds(0, half)], ld_sem.at[slot])
        c, h = place(j)

        @pl.when(j < 2)
        def _():
            src = own[w].at[pl.ds(pl.multiple_of(h * half, half), half)]
            load(src, rows_buf.at[slot, pl.ds(half, half)], ld_sem.at[slot])

        @pl.when(j >= 2)
        def _():
            load(of_core(gathered[w], j, core), rows_buf.at[slot, pl.ds(half, half)], ld_sem.at[slot])

    def rows_of(j):
        slot = j % 2
        pltpu.make_async_copy(rows_buf.at[slot], rows_buf.at[slot], ld_sem.at[slot]).wait()
        return rows_buf.at[slot]

    def pre_load(j, b):
        c, h = place(j)
        where = (1 - core) if b == 0 else core
        start = pl.multiple_of((c * CORES + where) * size + h * half, half)
        return pltpu.make_async_copy(
            pre.at[pl.ds(start, half)], pre_buf.at[j % 2, pl.ds(b * half, half)], pre_sem.at[j % 2]
        )

    def pair_sum(j):
        return remote(st_pair.at[pl.ds(pl.multiple_of(j % 2 * half, half), half)], pair_buf.at[j % 2], rsp_s.at[j % 2], rsp_r.at[j % 2], partner)

    def ring_sum(j):
        dev = lax.rem(me + n - CORES + 2 * CORES * (j % 2), n)
        return remote(st_ring.at[j - 4], ring_buf.at[j - 4], sum_s.at[j // 2 - 2], sum_r.at[j // 2 - 2], dev)

    pieces = ((0, half - LAST), (half - LAST, LAST))

    def chain_send(b, q):
        ref = (b, pl.ds(*pieces[q]))
        return remote(st_ring.at[ref], chain_buf.at[ref], sum_s.at[1], ch_r.at[q], left if b == 0 else right)

    barrier = pltpu.get_barrier_semaphore()
    for dev in (left, right, partner):
        pl.semaphore_signal(barrier, inc=1, device_id={"tp": dev}, device_id_type=MESH)
    pl.semaphore_wait(barrier, 3)

    for j in (2, 3, 4, 5):
        ring_own(DY, j).start()
    for j in (0, 1):
        to_partner(DY, j).start()
    for b in range(2):
        pre_load(0, b).start()
    load(w_down, wd, w_sem.at[0])
    load(w_in, wi, w_sem.at[1])

    @pl.loop(0, ff, step=64)
    def _(r):
        acc_down[pl.ds(pl.multiple_of(r, 64), 64)] = jnp.zeros((64, d), F32)

    @pl.loop(0, d, step=128)
    def _(r):
        acc_in[pl.ds(pl.multiple_of(r, 128), 128)] = jnp.zeros((128, ff), F32)

    start_rows(DY, 0)
    pltpu.make_async_copy(w_down, wd, w_sem.at[0]).wait()
    pltpu.make_async_copy(w_in, wi, w_sem.at[1]).wait()

    tile = 256

    @pl.loop(0, PAIRS)
    def _(i):
        slot = i % 2

        @pl.when(i == 1)
        def _():
            service(DY, 2)
            ring_own(X, 2).start()
            ring_own(X, 3).start()
            to_partner(X, 0).start()
            to_partner(X, 1).start()

        @pl.when(i == 3)
        def _():
            service(DY, 4)
            ring_own(X, 4).start()
            ring_own(X, 5).start()

        @pl.when(i == 5)
        def _():
            service(DY, 6)

        @pl.when(i < PAIRS - 1)
        def _():
            start_rows(DY, i + 1)
            for b in range(2):
                pre_load(i + 1, b).start()

        rows = rows_of(i)
        pltpu.make_async_copy(pre_buf.at[slot], pre_buf.at[slot], pre_sem.at[slot]).wait()

        @pl.loop(0, ff, step=tile)
        def _(f):
            fs = pl.ds(pl.multiple_of(f, tile), tile)
            dh = lax.dot_general(rows[...], wd[fs, :], NT, preferred_element_type=F32)
            h, slope = gelu_and_slope(pre_buf[slot, :, fs].astype(F32))
            dpre[i, :, fs] = (dh * slope).astype(BF16)
            hid[:, fs] = h.astype(BF16)

        @pl.when(i >= 2)
        def _():
            pair_sum(i - 2).wait_send()

        @pl.loop(0, d, step=2 * tile)
        def _(c):
            cs = pl.ds(pl.multiple_of(c, 2 * tile), 2 * tile)
            o = lax.dot_general(dpre[i, 0:half, :], wi[cs, :], NT, preferred_element_type=F32)
            st_pair[pl.ds(pl.multiple_of(slot * half, half), half), cs] = o.astype(BF16)

        pair_sum(i).start()

        @pl.loop(0, ff, step=tile)
        def _(f):
            fs = pl.ds(pl.multiple_of(f, tile), tile)

            for c in range(0, d, 2 * tile):
                acc_down[fs, c : c + 2 * tile] += lax.dot_general(
                    hid[:, fs], rows[:, c : c + 2 * tile], TN, preferred_element_type=F32
                )

        pair_sum(i).wait_recv()

        def mine(c):
            cs = pl.ds(pl.multiple_of(c, 2 * tile), 2 * tile)
            o = lax.dot_general(dpre[i, half : 2 * half, :], wi[cs, :], NT, preferred_element_type=F32)
            return cs, o + pair_buf[slot, :, cs].astype(F32)

        @pl.when(i < 4)
        def _():
            @pl.loop(0, d, step=2 * tile)
            def _(c):
                cs, o = mine(c)
                stash[i, :, cs] = o

        @pl.when(i >= 4)
        def _():
            @pl.loop(0, d, step=2 * tile)
            def _(c):
                cs, o = mine(c)
                st_ring[i - 4, :, cs] = o.astype(BF16)

            ring_sum(i).start()

    service(X, 2)
    start_rows(X, 0)
    for b in range(2):
        pair_sum(PAIRS - 2 + b).wait_send()

    @pl.loop(0, ff, step=32)
    def _(r):
        rs = pl.ds(pl.multiple_of(r, 32), 32)
        dw_down[rs] = acc_down[rs].astype(BF16)

    def hops(q):
        both = pl.ds(2 * q, 2)
        return remote(st_ring.at[both], ring_buf.at[both], sum_s.at[q], sum_r.at[q], right)

    def chain(b):
        @pl.loop(0, half, step=32)
        def _(r):
            rs = pl.ds(pl.multiple_of(r, 32), 32)
            st_ring[b, rs] = (stash[2 + b, rs] + ring_buf[2 + b, rs].astype(F32)).astype(BF16)

        for q in range(len(pieces)):
            chain_send(b, q).start()

    def direct(b):
        @pl.loop(0, half, step=32)
        def _(r):
            rs = pl.ds(pl.multiple_of(r, 32), 32)
            stash[1 - b, rs] += ring_buf[b, rs].astype(F32)

    @pl.loop(0, PAIRS)
    def _(i):
        @pl.when(i == 3)
        def _():
            service(X, 4)

        @pl.when(i == PAIRS - 2)
        def _():
            hops(0).wait()
            direct(0)
            direct(1)
            hops(1).wait_recv()
            chain(0)
            chain(1)
            service(X, 6)
            start_rows(X, i)
            start_rows(X, i + 1)

        @pl.when(i < PAIRS - 3)
        def _():
            start_rows(X, i + 1)

        rows = rows_of(i)

        @pl.loop(0, d, step=tile)
        def _(c):
            cs = pl.ds(pl.multiple_of(c, tile), tile)

            for f in range(0, ff, 2 * tile):
                acc_in[cs, f : f + 2 * tile] += lax.dot_general(
                    rows[:, cs], dpre[i, :, f : f + 2 * tile], TN, preferred_element_type=F32
                )

    @pl.loop(0, d, step=64)
    def _(r):
        rs = pl.ds(pl.multiple_of(r, 64), 64)
        dw_in[rs] = acc_in[rs].astype(BF16)

    ring_sent = x_all.at[pl.ds(0, PAIRS - 2)]
    remote(ring_sent, ring_sent, ring_s.at[0], ring_r.at[0, 0], right).wait_send()
    remote(x_all, x_all, pair_s.at[0], pair_r.at[0], partner).wait_send()

    for q in range(len(pieces)):
        both = chain_buf.at[:, pl.ds(*pieces[q])]
        remote(both, both, sum_s.at[1], ch_r.at[q], right).wait_recv()
        for b in range(2):

            @pl.loop(0, pieces[q][1], step=LAST)
            def _(r):
                rs = pl.ds(pl.multiple_of(pieces[q][0] + r, LAST), LAST)
                to = pl.ds(pl.multiple_of(b * half + pieces[q][0] + r, LAST), LAST)
                dx[to] = (stash[b, rs] + chain_buf[b, rs].astype(F32)).astype(BF16)

    remote(st_ring, ring_buf, sum_s.at[1], sum_r.at[1], left).wait_send()


def results(*refs):
    count = len(refs) // 2
    ins, outs, sem = refs[:count], refs[count : 2 * count], refs[-1]
    for a, b in zip(ins, outs):
        for start in range(0, a.shape[0], ROWS):
            rs = pl.ds(start, ROWS)
            pltpu.make_async_copy(a.at[rs], b.at[rs], sem.at[0]).start()
    for a, b in zip(ins, outs):
        pltpu.make_async_copy(a, b, sem.at[0]).wait()


def solution(mesh):
    n = mesh.shape["tp"]

    def step(x, dy, pre, w_in, w_down):
        (size, d), ff = x.shape, pre.shape[1]
        half = size // 2
        any_space = pl.BlockSpec(memory_space=pl.ANY)
        shapes = ((size, d), (d, ff), (ff, d))
        dma = pltpu.SemaphoreType.DMA
        outs = pl.pallas_call(
            functools.partial(kernel, n),
            out_shape=[pltpu.VMEM(s, BF16) for s in shapes]
            + [
                jax.ShapeDtypeStruct(s, BF16)
                for s in ((n, size, d), (n, size, d))
            ],
            in_specs=[any_space] * 5,
            out_specs=[pl.BlockSpec(memory_space=pltpu.VMEM)] * 3 + [any_space] * 2,
            scratch_shapes=[
                pltpu.VMEM((d, ff), F32),
                pltpu.VMEM((ff, d), F32),
                pltpu.VMEM((PAIRS, size, ff), BF16),
                pltpu.VMEM((4, half, d), F32),
                pltpu.VMEM((4, half, d), BF16),
                pltpu.VMEM((2, size, d), BF16),
                pltpu.VMEM((2, size, ff), BF16),
                pltpu.VMEM((size, ff), BF16),
                pltpu.VMEM((2, half, d), BF16),
                pltpu.VMEM((4, half, d), BF16),
                pltpu.VMEM((2, half, d), BF16),
                dma((1,)), dma((2, 3)), dma((1,)), dma((PAIRS // 2,)), dma((2,)), dma((2,)), dma((2,)), dma((2,)),
                dma((2,)), dma((2,)), dma((2,)), dma((2,)),
            ],
            compiler_params=pltpu.CompilerParams(collective_id=0, has_side_effects=True, vmem_limit_bytes=VMEM_LIMIT),
            name="mlp_backward",
        )(x, dy, pre, w_in, w_down)
        return tuple(
            pl.pallas_call(
                results,
                out_shape=[jax.ShapeDtypeStruct(s, BF16) for s in shapes],
                in_specs=[pl.BlockSpec(memory_space=pltpu.VMEM)] * 3,
                out_specs=[any_space] * 3,
                scratch_shapes=[dma((1,))],
                compiler_params=pltpu.CompilerParams(vmem_limit_bytes=2**20),
                name="results",
            )(*(pltpu.with_memory_space_constraint(o, pltpu.VMEM) for o in outs[:3]))
        )

    rows = P(("dp", "tp"), None)
    return jax.shard_map(
        step,
        mesh=mesh,
        in_specs=(rows, rows, P("dp", "tp"), P(None, "tp"), P("tp", None)),
        out_specs=(rows, P("dp", "tp"), rows),
        check_vma=False,
    )
```

```python
import functools

import jax
import jax.numpy as jnp
from jax import lax
from jax.experimental import pallas as pl
from jax.experimental.pallas import tpu as pltpu
from jax.sharding import PartitionSpec as P

MESH = pl.DeviceIdType.MESH
F32, BF16 = jnp.float32, jnp.bfloat16
CORES = 2
PAIRS = 8
LAST = 16
ROWS = 8
NT = (((1,), (1,)), ((), ()))
TN = (((0,), (0,)), ((), ()))
DY, X = 0, 1
VMEM_LIMIT = 53 * 2**20


def gelu_and_slope(p):
    c = 0.7978845608028654
    sq = p * p
    t = jnp.tanh(c * (p + 0.044715 * (sq * p)))
    cdf = 0.5 * (1.0 + t)
    slope = cdf + (0.5 * p) * (1.0 - t * t) * (c * (1.0 + 0.134145 * sq))
    return p * cdf, slope


def kernel(
    n, x, dy, pre, w_in, w_down,
    dx, dw_in, dw_down, x_all, dy_all,
    acc_in, acc_down, dpre, stash, st_ring, rows_buf, pre_buf, hid, pair_buf, ring_buf, chain_buf,
    sent, ring_r, pair_r, rsp_s, rsp_r, sum_r, ch_r, ld_sem,
):
    wi, wd, st_pair = dw_in, dw_down, dx
    me = lax.axis_index("tp")
    core = lax.rem(me, CORES)
    chip = me // CORES
    chips = n // CORES
    right = lax.rem(me + CORES, n)
    left = lax.rem(me + n - CORES, n)
    partner = me + 1 - 2 * core
    size, ff = x.shape[0], pre.shape[1]
    d = x.shape[1]
    half = size // 2

    def place(i):
        q, r = i // 2, i % 2
        odd = ((q + 1) // 2) % 2
        off = odd * (chips - 1 + 2 * r) + 2 * (q // 3)
        turned = (q // 2) * (1 - q // 3)
        return lax.rem(chip + off, chips), r + turned * (1 - 2 * r)

    def at(ref, shard, h):
        return ref.at[shard, pl.ds(pl.multiple_of(h * half, half), half)]

    def of_core(ref, i, k):
        c, h = place(i)
        return at(ref, c * CORES + k, h)

    own = (dy, x)
    gathered = (dy_all, x_all)

    def own_half(w, h):
        return own[w].at[pl.ds(h * half, half)]

    def remote(src, dst, s, r, dev):
        return pltpu.make_async_remote_copy(
            src_ref=src, dst_ref=dst, send_sem=s, recv_sem=r, device_id={"tp": dev}, device_id_type=MESH
        )

    def ring_sem(w, j):
        return ring_r.at[j // 2 - 1 if w == DY else 3 + j // 6]

    def pair_sem(j):
        return pair_r.at[(j // 2 + 1) // 2]

    def ring_own(w, j):
        h = {2: 0, 3: 1, 4: 1, 5: 0}[j]
        return remote(own_half(w, h), at(gathered[w], me, h), sent.at[0], ring_sem(w, j), right if j % 2 == 0 else left)

    def ring_relay(w, j):
        ref = of_core(gathered[w], j - 4, core)
        return remote(ref, ref, sent.at[0], ring_sem(w, j), right if j % 2 == 0 else left)

    def ring_send(w, j):
        return ring_own(w, j) if j < 6 else ring_relay(w, j)

    def to_partner(w, j):
        src = own_half(w, j) if j < 2 else of_core(gathered[w], j, core)
        return remote(src, of_core(gathered[w], j, core), sent.at[0], pair_sem(j), partner)

    def service(w, j):
        count = 4 if w == X and j == 2 else 2
        some = gathered[w].at[pl.ds(0, count // 2)]
        remote(some, some, sent.at[0], ring_sem(w, j), right).wait_recv()
        for q in range(j, j + count):
            if q < 4:
                ring_relay(w, q + 4).start()
            to_partner(w, q).start()

    def load(src, dst, sem):
        c = pltpu.make_async_copy(src, dst, sem)
        c.start()
        return c

    def start_rows(w, j):
        def arrived(pairs):
            some = gathered[w].at[pl.ds(0, pairs // 2)]
            remote(some, some, sent.at[0], pair_sem(j), partner).wait_recv()

        if w == DY:
            pl.when(j % 2 == 0)(lambda: arrived(2))
        else:
            for first, pairs in ((0, 2), (2, 4), (6, 2)):
                pl.when(j == first)(functools.partial(arrived, pairs))

        slot = j % 2
        load(of_core(gathered[w], j, 1 - core), rows_buf.at[slot, pl.ds(0, half)], ld_sem.at[slot])
        c, h = place(j)

        @pl.when(j < 2)
        def _():
            src = own[w].at[pl.ds(pl.multiple_of(h * half, half), half)]
            load(src, rows_buf.at[slot, pl.ds(half, half)], ld_sem.at[slot])

        @pl.when(j >= 2)
        def _():
            load(of_core(gathered[w], j, core), rows_buf.at[slot, pl.ds(half, half)], ld_sem.at[slot])

    def rows_of(j):
        slot = j % 2
        pltpu.make_async_copy(rows_buf.at[slot], rows_buf.at[slot], ld_sem.at[slot]).wait()
        return rows_buf.at[slot]

    def pre_load(j, b):
        c, h = place(j)
        where = (1 - core) if b == 0 else core
        start = pl.multiple_of((c * CORES + where) * size + h * half, half)
        return pltpu.make_async_copy(
            pre.at[pl.ds(start, half)], pre_buf.at[j % 2, pl.ds(b * half, half)], ld_sem.at[j % 2]
        )

    def pair_sum(j):
        return remote(st_pair.at[pl.ds(pl.multiple_of(j % 2 * half, half), half)], pair_buf.at[j % 2], rsp_s.at[0], rsp_r.at[j % 2], partner)

    def ring_sum(j):
        dev = lax.rem(me + n - CORES + 2 * CORES * (j % 2), n)
        return remote(st_ring.at[j - 4], ring_buf.at[j - 4], sent.at[3 - j // 2], sum_r.at[0], dev)

    pieces = ((0, half - LAST), (half - LAST, LAST))

    def chain_send(b, q):
        ref = (b, pl.ds(*pieces[q]))
        return remote(st_ring.at[ref], chain_buf.at[ref], sent.at[0], ch_r.at[q], left if b == 0 else right)

    barrier = pltpu.get_barrier_semaphore()
    for dev in (left, right, partner):
        pl.semaphore_signal(barrier, inc=1, device_id={"tp": dev}, device_id_type=MESH)
    pl.semaphore_wait(barrier, 3)

    for j in (2, 3, 4, 5):
        ring_own(DY, j).start()
    for j in (0, 1):
        to_partner(DY, j).start()
    for b in range(2):
        pre_load(0, b).start()
    load(w_down, wd, ld_sem.at[1])
    load(w_in, wi, ld_sem.at[1])

    @pl.loop(0, ff, step=64)
    def _(r):
        acc_down[pl.ds(pl.multiple_of(r, 64), 64)] = jnp.zeros((64, d), F32)

    @pl.loop(0, d, step=128)
    def _(r):
        acc_in[pl.ds(pl.multiple_of(r, 128), 128)] = jnp.zeros((128, ff), F32)

    start_rows(DY, 0)
    pltpu.make_async_copy(w_down, wd, ld_sem.at[1]).wait()
    pltpu.make_async_copy(w_in, wi, ld_sem.at[1]).wait()

    tile = 256

    @pl.loop(0, PAIRS)
    def _(i):
        slot = i % 2

        @pl.when(i == 1)
        def _():
            service(DY, 2)
            ring_own(X, 2).start()
            ring_own(X, 3).start()
            to_partner(X, 0).start()
            to_partner(X, 1).start()

        @pl.when(i == 3)
        def _():
            service(DY, 4)
            ring_own(X, 4).start()
            ring_own(X, 5).start()

        @pl.when(i == 5)
        def _():
            service(DY, 6)

        @pl.when(i < PAIRS - 1)
        def _():
            start_rows(DY, i + 1)
            for b in range(2):
                pre_load(i + 1, b).start()

        rows = rows_of(i)
        pltpu.make_async_copy(pre_buf.at[slot], pre_buf.at[slot], ld_sem.at[slot]).wait()

        @pl.loop(0, ff, step=tile)
        def _(f):
            fs = pl.ds(pl.multiple_of(f, tile), tile)
            dh = lax.dot_general(rows[...], wd[fs, :], NT, preferred_element_type=F32)
            h, slope = gelu_and_slope(pre_buf[slot, :, fs].astype(F32))
            dpre[i, :, fs] = (dh * slope).astype(BF16)
            hid[:, fs] = h.astype(BF16)

        @pl.when(i >= 1)
        def _():
            pair_sum(i - 1).wait_send()

        @pl.loop(0, d, step=2 * tile)
        def _(c):
            cs = pl.ds(pl.multiple_of(c, 2 * tile), 2 * tile)
            o = lax.dot_general(dpre[i, 0:half, :], wi[cs, :], NT, preferred_element_type=F32)
            st_pair[pl.ds(pl.multiple_of(slot * half, half), half), cs] = o.astype(BF16)

        pair_sum(i).start()

        @pl.loop(0, ff, step=tile)
        def _(f):
            fs = pl.ds(pl.multiple_of(f, tile), tile)

            for c in range(0, d, 2 * tile):
                acc_down[fs, c : c + 2 * tile] += lax.dot_general(
                    hid[:, fs], rows[:, c : c + 2 * tile], TN, preferred_element_type=F32
                )

        pair_sum(i).wait_recv()

        def mine(c):
            cs = pl.ds(pl.multiple_of(c, 2 * tile), 2 * tile)
            o = lax.dot_general(dpre[i, half : 2 * half, :], wi[cs, :], NT, preferred_element_type=F32)
            return cs, o + pair_buf[slot, :, cs].astype(F32)

        @pl.when(i < 4)
        def _():
            @pl.loop(0, d, step=2 * tile)
            def _(c):
                cs, o = mine(c)
                stash[i, :, cs] = o

        @pl.when(i >= 4)
        def _():
            @pl.loop(0, d, step=2 * tile)
            def _(c):
                cs, o = mine(c)
                st_ring[i - 4, :, cs] = o.astype(BF16)

            ring_sum(i).start()

    service(X, 2)
    start_rows(X, 0)
    pair_sum(PAIRS - 1).wait_send()

    @pl.loop(0, ff, step=32)
    def _(r):
        rs = pl.ds(pl.multiple_of(r, 32), 32)
        dw_down[rs] = acc_down[rs].astype(BF16)

    def chain(b):
        @pl.loop(0, half, step=32)
        def _(r):
            rs = pl.ds(pl.multiple_of(r, 32), 32)
            st_ring[b, rs] = (stash[2 + b, rs] + ring_buf[2 + b, rs].astype(F32)).astype(BF16)

        for q in range(len(pieces)):
            chain_send(b, q).start()

    def direct(b):
        @pl.loop(0, half, step=32)
        def _(r):
            rs = pl.ds(pl.multiple_of(r, 32), 32)
            stash[1 - b, rs] += ring_buf[b, rs].astype(F32)

    @pl.loop(0, PAIRS)
    def _(i):
        @pl.when(i == PAIRS - 2)
        def _():
            remote(st_ring, ring_buf, sent.at[0], sum_r.at[0], right).wait_recv()
            near = pl.ds(0, 2)
            remote(st_ring.at[near], ring_buf.at[near], sent.at[1], sum_r.at[0], right).wait_send()
            direct(0)
            direct(1)
            chain(0)
            chain(1)
            service(X, 6)
            start_rows(X, i)
            start_rows(X, i + 1)

        @pl.when(i < PAIRS - 3)
        def _():
            start_rows(X, i + 1)

        rows = rows_of(i)

        @pl.loop(0, d, step=tile)
        def _(c):
            cs = pl.ds(pl.multiple_of(c, tile), tile)

            for f in range(0, ff, 2 * tile):
                acc_in[cs, f : f + 2 * tile] += lax.dot_general(
                    rows[:, cs], dpre[i, :, f : f + 2 * tile], TN, preferred_element_type=F32
                )

    @pl.loop(0, d, step=64)
    def _(r):
        rs = pl.ds(pl.multiple_of(r, 64), 64)
        dw_in[rs] = acc_in[rs].astype(BF16)

    for q in range(len(pieces)):
        both = chain_buf.at[:, pl.ds(*pieces[q])]
        remote(both, both, sent.at[0], ch_r.at[q], right).wait_recv()
        for b in range(2):

            @pl.loop(0, pieces[q][1], step=LAST)
            def _(r):
                rs = pl.ds(pl.multiple_of(pieces[q][0] + r, LAST), LAST)
                to = pl.ds(pl.multiple_of(b * half + pieces[q][0] + r, LAST), LAST)
                dx[to] = (stash[b, rs] + chain_buf[b, rs].astype(F32)).astype(BF16)

    for some in (x_all.at[pl.ds(0, PAIRS - 2)], x_all, st_ring):
        remote(some, some, sent.at[0], sum_r.at[0], right).wait_send()


def results(*refs):
    count = len(refs) // 2
    ins, outs, sem = refs[:count], refs[count : 2 * count], refs[-1]
    todo = [(a, b, start) for a, b in zip(ins, outs) for start in range(0, a.shape[0], ROWS)]
    for a, b, start in sorted(todo, key=lambda t: t[2] / t[0].shape[0]):
        rs = pl.ds(start, ROWS)
        pltpu.make_async_copy(a.at[rs], b.at[rs], sem.at[0]).start()
    for a, b in zip(ins, outs):
        pltpu.make_async_copy(a, b, sem.at[0]).wait()


def solution(mesh):
    n = mesh.shape["tp"]

    def step(x, dy, pre, w_in, w_down):
        (size, d), ff = x.shape, pre.shape[1]
        half = size // 2
        any_space = pl.BlockSpec(memory_space=pl.ANY)
        shapes = ((size, d), (d, ff), (ff, d))
        dma = pltpu.SemaphoreType.DMA
        outs = pl.pallas_call(
            functools.partial(kernel, n),
            out_shape=[pltpu.VMEM(s, BF16) for s in shapes]
            + [
                jax.ShapeDtypeStruct(s, BF16)
                for s in ((n, size, d), (n, size, d))
            ],
            in_specs=[any_space] * 5,
            out_specs=[pl.BlockSpec(memory_space=pltpu.VMEM)] * 3 + [any_space] * 2,
            scratch_shapes=[
                pltpu.VMEM((d, ff), F32),
                pltpu.VMEM((ff, d), F32),
                pltpu.VMEM((PAIRS, size, ff), BF16),
                pltpu.VMEM((4, half, d), F32),
                pltpu.VMEM((4, half, d), BF16),
                pltpu.VMEM((2, size, d), BF16),
                pltpu.VMEM((2, size, ff), BF16),
                pltpu.VMEM((size, ff), BF16),
                pltpu.VMEM((2, half, d), BF16),
                pltpu.VMEM((4, half, d), BF16),
                pltpu.VMEM((2, half, d), BF16),
                dma((2,)), dma((5,)), dma((3,)), dma((1,)), dma((2,)), dma((1,)), dma((2,)), dma((2,)),
            ],
            compiler_params=pltpu.CompilerParams(collective_id=0, has_side_effects=True, vmem_limit_bytes=VMEM_LIMIT),
            name="mlp_backward",
        )(x, dy, pre, w_in, w_down)
        return tuple(
            pl.pallas_call(
                results,
                out_shape=[jax.ShapeDtypeStruct(s, BF16) for s in shapes],
                in_specs=[pl.BlockSpec(memory_space=pltpu.VMEM)] * 3,
                out_specs=[any_space] * 3,
                scratch_shapes=[dma((1,))],
                compiler_params=pltpu.CompilerParams(vmem_limit_bytes=2**20),
                name="results",
            )(*(pltpu.with_memory_space_constraint(o, pltpu.VMEM) for o in outs[:3]))
        )

    rows = P(("dp", "tp"), None)
    return jax.shard_map(
        step,
        mesh=mesh,
        in_specs=(rows, rows, P("dp", "tp"), P(None, "tp"), P("tp", None)),
        out_specs=(rows, P("dp", "tp"), rows),
        check_vma=False,
    )
```

```python
import functools

import jax
import jax.numpy as jnp
from jax import lax
from jax.experimental import pallas as pl
from jax.experimental.pallas import tpu as pltpu
from jax.sharding import PartitionSpec as P

MESH = pl.DeviceIdType.MESH
F32, BF16 = jnp.float32, jnp.bfloat16
CORES = 2
PAIRS = 8
LAST = 16
ROWS = 8
NT = (((1,), (1,)), ((), ()))
TN = (((0,), (0,)), ((), ()))
DY, X = 0, 1
VMEM_LIMIT = 53 * 2**20


def gelu_and_slope(p):
    c = 0.7978845608028654
    sq = p * p
    t = jnp.tanh(c * (p + 0.044715 * (sq * p)))
    cdf = 0.5 * (1.0 + t)
    slope = cdf + (0.5 * p) * (1.0 - t * t) * (c * (1.0 + 0.134145 * sq))
    return p * cdf, slope


def kernel(
    n, x, dy, pre, w_in, w_down,
    dx, dw_in, dw_down, x_all, dy_all,
    acc_in, acc_down, dpre, stash, st_ring, rows_buf, pre_buf, hid, pair_buf, ring_buf, chain_buf,
    sent, ring_r, pair_r, rsp_s, rsp_r, sum_r, ch_r, ld_sem,
):
    wi, wd, st_pair = dw_in, dw_down, dx
    me = lax.axis_index("tp")
    core = lax.rem(me, CORES)
    chip = me // CORES
    chips = n // CORES
    right = lax.rem(me + CORES, n)
    left = lax.rem(me + n - CORES, n)
    partner = me + 1 - 2 * core
    size, ff = x.shape[0], pre.shape[1]
    d = x.shape[1]
    half = size // 2

    def place(i):
        q, r = i // 2, i % 2
        odd = ((q + 1) // 2) % 2
        off = odd * (chips - 1 + 2 * r) + 2 * (q // 3)
        turned = (q // 2) * (1 - q // 3)
        return lax.rem(chip + off, chips), r + turned * (1 - 2 * r)

    def at(ref, shard, h):
        return ref.at[shard, pl.ds(pl.multiple_of(h * half, half), half)]

    def of_core(ref, i, k):
        c, h = place(i)
        return at(ref, c * CORES + k, h)

    own = (dy, x)
    gathered = (dy_all, x_all)

    def own_half(w, h):
        return own[w].at[pl.ds(h * half, half)]

    def remote(src, dst, s, r, dev):
        return pltpu.make_async_remote_copy(
            src_ref=src, dst_ref=dst, send_sem=s, recv_sem=r, device_id={"tp": dev}, device_id_type=MESH
        )

    def ring_sem(w, j):
        return ring_r.at[j // 2 - 1 if w == DY else 3 - 3 * (j // 6)]

    def pair_sem(w, j):
        return pair_r.at[j // 2 % 2 if w == DY else 1 - j // 6]

    def ring_own(w, j):
        h = {2: 0, 3: 1, 4: 1, 5: 0}[j]
        return remote(own_half(w, h), at(gathered[w], me, h), sent.at[0], ring_sem(w, j), right if j % 2 == 0 else left)

    def ring_relay(w, j):
        ref = of_core(gathered[w], j - 4, core)
        return remote(ref, ref, sent.at[0], ring_sem(w, j), right if j % 2 == 0 else left)

    def ring_send(w, j):
        return ring_own(w, j) if j < 6 else ring_relay(w, j)

    def to_partner(w, j):
        src = own_half(w, j) if j < 2 else of_core(gathered[w], j, core)
        return remote(src, of_core(gathered[w], j, core), sent.at[0], pair_sem(w, j), partner)

    def service(w, j):
        count = 4 if w == X and j == 2 else 2
        some = gathered[w].at[pl.ds(0, count // 2)]
        remote(some, some, sent.at[0], ring_sem(w, j), right).wait_recv()
        for q in range(j, j + count):
            if q < 4:
                ring_relay(w, q + 4).start()
            to_partner(w, q).start()

    def load(src, dst, sem):
        c = pltpu.make_async_copy(src, dst, sem)
        c.start()
        return c

    def start_rows(w, j):
        def arrived(pairs):
            some = gathered[w].at[pl.ds(0, pairs // 2)]
            remote(some, some, sent.at[0], pair_sem(w, j), partner).wait_recv()

        if w == DY:
            pl.when(j % 2 == 0)(lambda: arrived(2))
        else:
            for first, pairs in ((0, 6), (6, 2)):
                pl.when(j == first)(functools.partial(arrived, pairs))

        slot = j % 2
        load(of_core(gathered[w], j, 1 - core), rows_buf.at[slot, pl.ds(0, half)], ld_sem.at[slot])
        c, h = place(j)

        @pl.when(j < 2)
        def _():
            src = own[w].at[pl.ds(pl.multiple_of(h * half, half), half)]
            load(src, rows_buf.at[slot, pl.ds(half, half)], ld_sem.at[slot])

        @pl.when(j >= 2)
        def _():
            load(of_core(gathered[w], j, core), rows_buf.at[slot, pl.ds(half, half)], ld_sem.at[slot])

    def rows_of(j):
        slot = j % 2
        pltpu.make_async_copy(rows_buf.at[slot], rows_buf.at[slot], ld_sem.at[slot]).wait()
        return rows_buf.at[slot]

    def pre_load(j, b):
        c, h = place(j)
        where = (1 - core) if b == 0 else core
        start = pl.multiple_of((c * CORES + where) * size + h * half, half)
        return pltpu.make_async_copy(
            pre.at[pl.ds(start, half)], pre_buf.at[j % 2, pl.ds(b * half, half)], ld_sem.at[j % 2]
        )

    def pair_sum(j):
        return remote(st_pair.at[pl.ds(pl.multiple_of(j % 2 * half, half), half)], pair_buf.at[j % 2], rsp_s.at[0], rsp_r.at[j % 2], partner)

    def ring_sum(j):
        dev = lax.rem(me + n - CORES + 2 * CORES * (j % 2), n)
        return remote(st_ring.at[j - 4], ring_buf.at[j - 4], sent.at[3 - j // 2], sum_r.at[0], dev)

    pieces = ((0, half - LAST), (half - LAST, LAST))

    def chain_send(b, q):
        ref = (b, pl.ds(*pieces[q]))
        return remote(st_ring.at[ref], chain_buf.at[ref], sent.at[0], ch_r.at[q], left if b == 0 else right)

    barrier = pltpu.get_barrier_semaphore()
    for dev in (left, right, partner):
        pl.semaphore_signal(barrier, inc=1, device_id={"tp": dev}, device_id_type=MESH)
    pl.semaphore_wait(barrier, 3)

    for j in (2, 3, 4, 5):
        ring_own(DY, j).start()
    for j in (0, 1):
        to_partner(DY, j).start()
    for b in range(2):
        pre_load(0, b).start()
    load(w_down, wd, ld_sem.at[1])
    load(w_in, wi, ld_sem.at[1])

    @pl.loop(0, ff, step=64)
    def _(r):
        acc_down[pl.ds(pl.multiple_of(r, 64), 64)] = jnp.zeros((64, d), F32)

    @pl.loop(0, d, step=128)
    def _(r):
        acc_in[pl.ds(pl.multiple_of(r, 128), 128)] = jnp.zeros((128, ff), F32)

    start_rows(DY, 0)
    pltpu.make_async_copy(w_down, wd, ld_sem.at[1]).wait()
    pltpu.make_async_copy(w_in, wi, ld_sem.at[1]).wait()

    tile = 256

    @pl.loop(0, PAIRS)
    def _(i):
        slot = i % 2

        @pl.when(i == 1)
        def _():
            service(DY, 2)
            ring_own(X, 2).start()
            ring_own(X, 3).start()

        @pl.when(i == 3)
        def _():
            service(DY, 4)
            ring_own(X, 4).start()
            ring_own(X, 5).start()

        @pl.when(i == 5)
        def _():
            service(DY, 6)

        @pl.when(i < PAIRS - 1)
        def _():
            start_rows(DY, i + 1)
            for b in range(2):
                pre_load(i + 1, b).start()

        rows = rows_of(i)
        pltpu.make_async_copy(pre_buf.at[slot], pre_buf.at[slot], ld_sem.at[slot]).wait()

        @pl.loop(0, ff, step=tile)
        def _(f):
            fs = pl.ds(pl.multiple_of(f, tile), tile)
            dh = lax.dot_general(rows[...], wd[fs, :], NT, preferred_element_type=F32)
            h, slope = gelu_and_slope(pre_buf[slot, :, fs].astype(F32))
            dpre[i, :, fs] = (dh * slope).astype(BF16)
            hid[:, fs] = h.astype(BF16)

        @pl.when(i >= 1)
        def _():
            pair_sum(i - 1).wait_send()

        @pl.loop(0, d, step=2 * tile)
        def _(c):
            cs = pl.ds(pl.multiple_of(c, 2 * tile), 2 * tile)
            o = lax.dot_general(dpre[i, 0:half, :], wi[cs, :], NT, preferred_element_type=F32)
            st_pair[pl.ds(pl.multiple_of(slot * half, half), half), cs] = o.astype(BF16)

        pair_sum(i).start()

        @pl.loop(0, ff, step=tile)
        def _(f):
            fs = pl.ds(pl.multiple_of(f, tile), tile)

            for c in range(0, d, 2 * tile):
                acc_down[fs, c : c + 2 * tile] += lax.dot_general(
                    hid[:, fs], rows[:, c : c + 2 * tile], TN, preferred_element_type=F32
                )

        pair_sum(i).wait_recv()

        def mine(c):
            cs = pl.ds(pl.multiple_of(c, 2 * tile), 2 * tile)
            o = lax.dot_general(dpre[i, half : 2 * half, :], wi[cs, :], NT, preferred_element_type=F32)
            return cs, o + pair_buf[slot, :, cs].astype(F32)

        @pl.when(i < 4)
        def _():
            @pl.loop(0, d, step=2 * tile)
            def _(c):
                cs, o = mine(c)
                stash[i, :, cs] = o

        @pl.when(i >= 4)
        def _():
            @pl.loop(0, d, step=2 * tile)
            def _(c):
                cs, o = mine(c)
                st_ring[i - 4, :, cs] = o.astype(BF16)

            ring_sum(i).start()

    to_partner(X, 0).start()
    to_partner(X, 1).start()
    service(X, 2)
    start_rows(X, 0)
    pair_sum(PAIRS - 1).wait_send()

    @pl.loop(0, ff, step=32)
    def _(r):
        rs = pl.ds(pl.multiple_of(r, 32), 32)
        dw_down[rs] = acc_down[rs].astype(BF16)

    def chain(b):
        @pl.loop(0, half, step=32)
        def _(r):
            rs = pl.ds(pl.multiple_of(r, 32), 32)
            st_ring[b, rs] = (stash[2 + b, rs] + ring_buf[2 + b, rs].astype(F32)).astype(BF16)

        for q in range(len(pieces)):
            chain_send(b, q).start()

    def direct(b):
        @pl.loop(0, half, step=32)
        def _(r):
            rs = pl.ds(pl.multiple_of(r, 32), 32)
            stash[1 - b, rs] += ring_buf[b, rs].astype(F32)

    @pl.loop(0, PAIRS)
    def _(i):
        @pl.when(i == PAIRS - 2)
        def _():
            remote(st_ring, ring_buf, sent.at[0], sum_r.at[0], right).wait_recv()
            near = pl.ds(0, 2)
            remote(st_ring.at[near], ring_buf.at[near], sent.at[1], sum_r.at[0], right).wait_send()
            direct(0)
            direct(1)
            chain(0)
            chain(1)
            service(X, 6)
            start_rows(X, i)
            start_rows(X, i + 1)

        @pl.when(i < PAIRS - 3)
        def _():
            start_rows(X, i + 1)

        rows = rows_of(i)

        @pl.loop(0, d, step=tile)
        def _(c):
            cs = pl.ds(pl.multiple_of(c, tile), tile)

            for f in range(0, ff, 2 * tile):
                acc_in[cs, f : f + 2 * tile] += lax.dot_general(
                    rows[:, cs], dpre[i, :, f : f + 2 * tile], TN, preferred_element_type=F32
                )

    @pl.loop(0, d, step=64)
    def _(r):
        rs = pl.ds(pl.multiple_of(r, 64), 64)
        dw_in[rs] = acc_in[rs].astype(BF16)

    for q in range(len(pieces)):
        both = chain_buf.at[:, pl.ds(*pieces[q])]
        remote(both, both, sent.at[0], ch_r.at[q], right).wait_recv()
        for b in range(2):

            @pl.loop(0, pieces[q][1], step=LAST)
            def _(r):
                rs = pl.ds(pl.multiple_of(pieces[q][0] + r, LAST), LAST)
                to = pl.ds(pl.multiple_of(b * half + pieces[q][0] + r, LAST), LAST)
                dx[to] = (stash[b, rs] + chain_buf[b, rs].astype(F32)).astype(BF16)

    for some in (x_all.at[pl.ds(0, PAIRS - 2)], x_all, st_ring):
        remote(some, some, sent.at[0], sum_r.at[0], right).wait_send()


def results(*refs):
    count = len(refs) // 2
    ins, outs, sem = refs[:count], refs[count : 2 * count], refs[-1]
    todo = [(a, b, start) for a, b in zip(ins, outs) for start in range(0, a.shape[0], ROWS)]
    for a, b, start in sorted(todo, key=lambda t: t[2] / t[0].shape[0]):
        rs = pl.ds(start, ROWS)
        pltpu.make_async_copy(a.at[rs], b.at[rs], sem.at[0]).start()
    for a, b in zip(ins, outs):
        pltpu.make_async_copy(a, b, sem.at[0]).wait()


def solution(mesh):
    n = mesh.shape["tp"]

    def step(x, dy, pre, w_in, w_down):
        (size, d), ff = x.shape, pre.shape[1]
        half = size // 2
        any_space = pl.BlockSpec(memory_space=pl.ANY)
        shapes = ((size, d), (d, ff), (ff, d))
        dma = pltpu.SemaphoreType.DMA
        outs = pl.pallas_call(
            functools.partial(kernel, n),
            out_shape=[pltpu.VMEM(s, BF16) for s in shapes]
            + [
                jax.ShapeDtypeStruct(s, BF16)
                for s in ((n, size, d), (n, size, d))
            ],
            in_specs=[any_space] * 5,
            out_specs=[pl.BlockSpec(memory_space=pltpu.VMEM)] * 3 + [any_space] * 2,
            scratch_shapes=[
                pltpu.VMEM((d, ff), F32),
                pltpu.VMEM((ff, d), F32),
                pltpu.VMEM((PAIRS, size, ff), BF16),
                pltpu.VMEM((4, half, d), F32),
                pltpu.VMEM((4, half, d), BF16),
                pltpu.VMEM((2, size, d), BF16),
                pltpu.VMEM((2, size, ff), BF16),
                pltpu.VMEM((size, ff), BF16),
                pltpu.VMEM((2, half, d), BF16),
                pltpu.VMEM((4, half, d), BF16),
                pltpu.VMEM((2, half, d), BF16),
                dma((2,)), dma((4,)), dma((2,)), dma((1,)), dma((2,)), dma((1,)), dma((2,)), dma((2,)),
            ],
            compiler_params=pltpu.CompilerParams(collective_id=0, has_side_effects=True, vmem_limit_bytes=VMEM_LIMIT),
            name="mlp_backward",
        )(x, dy, pre, w_in, w_down)
        return tuple(
            pl.pallas_call(
                results,
                out_shape=[jax.ShapeDtypeStruct(s, BF16) for s in shapes],
                in_specs=[pl.BlockSpec(memory_space=pltpu.VMEM)] * 3,
                out_specs=[any_space] * 3,
                scratch_shapes=[dma((1,))],
                compiler_params=pltpu.CompilerParams(vmem_limit_bytes=2**20),
                name="results",
            )(*(pltpu.with_memory_space_constraint(o, pltpu.VMEM) for o in outs[:3]))
        )

    rows = P(("dp", "tp"), None)
    return jax.shard_map(
        step,
        mesh=mesh,
        in_specs=(rows, rows, P("dp", "tp"), P(None, "tp"), P("tp", None)),
        out_specs=(rows, P("dp", "tp"), rows),
        check_vma=False,
    )
```

```python
import functools

import jax
import jax.numpy as jnp
from jax import lax
from jax.experimental import pallas as pl
from jax.experimental.pallas import tpu as pltpu
from jax.sharding import PartitionSpec as P

MESH = pl.DeviceIdType.MESH
F32, BF16 = jnp.float32, jnp.bfloat16
CORES = 2
PAIRS = 8
LAST = 16
ROWS = 8
NT = (((1,), (1,)), ((), ()))
TN = (((0,), (0,)), ((), ()))
DY, X = 0, 1
VMEM_LIMIT = 53 * 2**20


def gelu_and_slope(p):
    c = 0.7978845608028654
    sq = p * p
    t = jnp.tanh(c * (p + 0.044715 * (sq * p)))
    cdf = 0.5 * (1.0 + t)
    slope = cdf + (0.5 * p) * (1.0 - t * t) * (c * (1.0 + 0.134145 * sq))
    return p * cdf, slope


def kernel(
    n, x, dy, pre, w_in, w_down,
    dx, dw_in, dw_down, x_all, dy_all,
    acc_in, acc_down, dpre, stash, st_ring, rows_buf, pre_buf, hid, pair_buf, ring_buf, chain_buf,
    sent, ring_r, pair_r, rsp_s, rsp_r, sum_r, ch_r, ld_sem,
):
    wi, wd, st_pair = dw_in, dw_down, dx
    me = lax.axis_index("tp")
    core = lax.rem(me, CORES)
    chip = me // CORES
    chips = n // CORES
    right = lax.rem(me + CORES, n)
    left = lax.rem(me + n - CORES, n)
    partner = me + 1 - 2 * core
    size, ff = x.shape[0], pre.shape[1]
    d = x.shape[1]
    half = size // 2

    def place(i):
        q, r = i // 2, i % 2
        odd = ((q + 1) // 2) % 2
        off = odd * (chips - 1 + 2 * r) + 2 * (q // 3)
        turned = (q // 2) * (1 - q // 3)
        return lax.rem(chip + off, chips), r + turned * (1 - 2 * r)

    def at(ref, shard, h):
        return ref.at[shard, pl.ds(pl.multiple_of(h * half, half), half)]

    def of_core(ref, i, k):
        c, h = place(i)
        return at(ref, c * CORES + k, h)

    own = (dy, x)
    gathered = (dy_all, x_all)

    def own_half(w, h):
        return own[w].at[pl.ds(h * half, half)]

    def remote(src, dst, s, r, dev):
        return pltpu.make_async_remote_copy(
            src_ref=src, dst_ref=dst, send_sem=s, recv_sem=r, device_id={"tp": dev}, device_id_type=MESH
        )

    def ring_sem(w, j):
        return ring_r.at[j // 2 - 1 if w == DY else 3 - 3 * (j // 6)]

    def pair_sem(w, j):
        return pair_r.at[j // 2 % 2 if w == DY else 1 - j // 6]

    def ring_own(w, j):
        h = {2: 0, 3: 1, 4: 1, 5: 0}[j]
        return remote(own_half(w, h), at(gathered[w], me, h), sent.at[0], ring_sem(w, j), right if j % 2 == 0 else left)

    def ring_relay(w, j):
        ref = of_core(gathered[w], j - 4, core)
        return remote(ref, ref, sent.at[0], ring_sem(w, j), right if j % 2 == 0 else left)

    def ring_send(w, j):
        return ring_own(w, j) if j < 6 else ring_relay(w, j)

    def to_partner(w, j):
        src = own_half(w, j) if j < 2 else of_core(gathered[w], j, core)
        return remote(src, of_core(gathered[w], j, core), sent.at[0], pair_sem(w, j), partner)

    def service(w, j):
        count = 4 if w == X and j == 2 else 2
        some = gathered[w].at[pl.ds(0, count // 2)]
        remote(some, some, sent.at[0], ring_sem(w, j), right).wait_recv()
        for q in range(j, j + count):
            if q < 4:
                ring_relay(w, q + 4).start()
            to_partner(w, q).start()

    def load(src, dst, sem):
        c = pltpu.make_async_copy(src, dst, sem)
        c.start()
        return c

    def start_rows(w, j):
        def arrived(pairs):
            some = gathered[w].at[pl.ds(0, pairs // 2)]
            remote(some, some, sent.at[0], pair_sem(w, j), partner).wait_recv()

        if w == DY:
            pl.when(j % 2 == 0)(lambda: arrived(2))
        else:
            for first, pairs in ((0, 6), (6, 2)):
                pl.when(j == first)(functools.partial(arrived, pairs))

        slot = j % 2
        load(of_core(gathered[w], j, 1 - core), rows_buf.at[slot, pl.ds(0, half)], ld_sem.at[slot])
        c, h = place(j)

        @pl.when(j < 2)
        def _():
            src = own[w].at[pl.ds(pl.multiple_of(h * half, half), half)]
            load(src, rows_buf.at[slot, pl.ds(half, half)], ld_sem.at[slot])

        @pl.when(j >= 2)
        def _():
            load(of_core(gathered[w], j, core), rows_buf.at[slot, pl.ds(half, half)], ld_sem.at[slot])

    def rows_of(j):
        slot = j % 2
        pltpu.make_async_copy(rows_buf.at[slot], rows_buf.at[slot], ld_sem.at[slot]).wait()
        return rows_buf.at[slot]

    def pre_load(j, b):
        c, h = place(j)
        where = (1 - core) if b == 0 else core
        start = pl.multiple_of((c * CORES + where) * size + h * half, half)
        return pltpu.make_async_copy(
            pre.at[pl.ds(start, half)], pre_buf.at[j % 2, pl.ds(b * half, half)], ld_sem.at[j % 2]
        )

    def pair_sum(j):
        return remote(st_pair.at[pl.ds(pl.multiple_of(j % 2 * half, half), half)], pair_buf.at[j % 2], rsp_s.at[0], rsp_r.at[j % 2], partner)

    def ring_sum(j):
        dev = lax.rem(me + n - CORES + 2 * CORES * (j % 2), n)
        return remote(st_ring.at[j - 4], ring_buf.at[j - 4], sent.at[3 - j // 2], sum_r.at[0], dev)

    pieces = ((0, half - LAST), (half - LAST, LAST))

    def chain_send(b, q):
        ref = (b, pl.ds(*pieces[q]))
        return remote(st_ring.at[ref], chain_buf.at[ref], sent.at[0], ch_r.at[q], left if b == 0 else right)

    barrier = pltpu.get_barrier_semaphore()
    for dev in (partner, left, right):
        pl.semaphore_signal(barrier, inc=1, device_id={"tp": dev}, device_id_type=MESH)
    pl.semaphore_wait(barrier, 3)

    for j in (2, 3, 4, 5):
        ring_own(DY, j).start()
    for j in (0, 1):
        to_partner(DY, j).start()
    for b in range(2):
        pre_load(0, b).start()
    load(w_down, wd, ld_sem.at[1])
    load(w_in, wi, ld_sem.at[1])

    @pl.loop(0, ff, step=64)
    def _(r):
        acc_down[pl.ds(pl.multiple_of(r, 64), 64)] = jnp.zeros((64, d), F32)

    @pl.loop(0, d, step=128)
    def _(r):
        acc_in[pl.ds(pl.multiple_of(r, 128), 128)] = jnp.zeros((128, ff), F32)

    start_rows(DY, 0)
    pltpu.make_async_copy(w_down, wd, ld_sem.at[1]).wait()
    pltpu.make_async_copy(w_in, wi, ld_sem.at[1]).wait()

    tile = 256

    @pl.loop(0, PAIRS)
    def _(i):
        slot = i % 2

        @pl.when(i == 1)
        def _():
            service(DY, 2)
            ring_own(X, 2).start()
            ring_own(X, 3).start()

        @pl.when(i == 3)
        def _():
            service(DY, 4)
            ring_own(X, 4).start()
            ring_own(X, 5).start()

        @pl.when(i == 5)
        def _():
            service(DY, 6)

        @pl.when(i < PAIRS - 1)
        def _():
            start_rows(DY, i + 1)
            for b in range(2):
                pre_load(i + 1, b).start()

        rows = rows_of(i)
        pltpu.make_async_copy(pre_buf.at[slot], pre_buf.at[slot], ld_sem.at[slot]).wait()

        @pl.loop(0, ff, step=tile)
        def _(f):
            fs = pl.ds(pl.multiple_of(f, tile), tile)
            dh = lax.dot_general(rows[...], wd[fs, :], NT, preferred_element_type=F32)
            h, slope = gelu_and_slope(pre_buf[slot, :, fs].astype(F32))
            dpre[i, :, fs] = (dh * slope).astype(BF16)
            hid[:, fs] = h.astype(BF16)

        @pl.when(i >= 1)
        def _():
            pair_sum(i - 1).wait_send()

        @pl.loop(0, d, step=2 * tile)
        def _(c):
            cs = pl.ds(pl.multiple_of(c, 2 * tile), 2 * tile)
            o = lax.dot_general(dpre[i, 0:half, :], wi[cs, :], NT, preferred_element_type=F32)
            st_pair[pl.ds(pl.multiple_of(slot * half, half), half), cs] = o.astype(BF16)

        pair_sum(i).start()

        @pl.loop(0, ff, step=tile)
        def _(f):
            fs = pl.ds(pl.multiple_of(f, tile), tile)

            for c in range(0, d, 2 * tile):
                acc_down[fs, c : c + 2 * tile] += lax.dot_general(
                    hid[:, fs], rows[:, c : c + 2 * tile], TN, preferred_element_type=F32
                )

        pair_sum(i).wait_recv()

        def mine(c):
            cs = pl.ds(pl.multiple_of(c, 2 * tile), 2 * tile)
            o = lax.dot_general(dpre[i, half : 2 * half, :], wi[cs, :], NT, preferred_element_type=F32)
            return cs, o + pair_buf[slot, :, cs].astype(F32)

        @pl.when(i < 4)
        def _():
            @pl.loop(0, d, step=2 * tile)
            def _(c):
                cs, o = mine(c)
                stash[i, :, cs] = o

        @pl.when(i >= 4)
        def _():
            @pl.loop(0, d, step=2 * tile)
            def _(c):
                cs, o = mine(c)
                st_ring[i - 4, :, cs] = o.astype(BF16)

            ring_sum(i).start()

    to_partner(X, 0).start()
    to_partner(X, 1).start()
    service(X, 2)
    start_rows(X, 0)
    pair_sum(PAIRS - 1).wait_send()

    @pl.loop(0, ff, step=32)
    def _(r):
        rs = pl.ds(pl.multiple_of(r, 32), 32)
        dw_down[rs] = acc_down[rs].astype(BF16)

    def chain(b):
        @pl.loop(0, half, step=32)
        def _(r):
            rs = pl.ds(pl.multiple_of(r, 32), 32)
            st_ring[b, rs] = (stash[2 + b, rs] + ring_buf[2 + b, rs].astype(F32)).astype(BF16)

        for q in range(len(pieces)):
            chain_send(b, q).start()

    def direct(b):
        @pl.loop(0, half, step=32)
        def _(r):
            rs = pl.ds(pl.multiple_of(r, 32), 32)
            stash[1 - b, rs] += ring_buf[b, rs].astype(F32)

    @pl.loop(0, PAIRS)
    def _(i):
        @pl.when(i == PAIRS - 2)
        def _():
            remote(st_ring, ring_buf, sent.at[0], sum_r.at[0], right).wait_recv()
            near = pl.ds(0, 2)
            remote(st_ring.at[near], ring_buf.at[near], sent.at[1], sum_r.at[0], right).wait_send()
            direct(0)
            direct(1)
            chain(0)
            chain(1)
            service(X, 6)
            start_rows(X, i)
            start_rows(X, i + 1)

        @pl.when(i < PAIRS - 3)
        def _():
            start_rows(X, i + 1)

        rows = rows_of(i)

        @pl.loop(0, d, step=tile)
        def _(c):
            cs = pl.ds(pl.multiple_of(c, tile), tile)

            for f in range(0, ff, 2 * tile):
                acc_in[cs, f : f + 2 * tile] += lax.dot_general(
                    rows[:, cs], dpre[i, :, f : f + 2 * tile], TN, preferred_element_type=F32
                )

    @pl.loop(0, d, step=64)
    def _(r):
        rs = pl.ds(pl.multiple_of(r, 64), 64)
        dw_in[rs] = acc_in[rs].astype(BF16)

    for q in range(len(pieces)):
        both = chain_buf.at[:, pl.ds(*pieces[q])]
        remote(both, both, sent.at[0], ch_r.at[q], right).wait_recv()
        for b in range(2):

            @pl.loop(0, pieces[q][1], step=LAST)
            def _(r):
                rs = pl.ds(pl.multiple_of(pieces[q][0] + r, LAST), LAST)
                to = pl.ds(pl.multiple_of(b * half + pieces[q][0] + r, LAST), LAST)
                dx[to] = (stash[b, rs] + chain_buf[b, rs].astype(F32)).astype(BF16)

    for some in (x_all.at[pl.ds(0, PAIRS - 2)], x_all, st_ring):
        remote(some, some, sent.at[0], sum_r.at[0], right).wait_send()


def results(*refs):
    count = len(refs) // 2
    ins, outs, sem = refs[:count], refs[count : 2 * count], refs[-1]
    todo = [(a, b, start) for a, b in zip(ins, outs) for start in range(0, a.shape[0], ROWS)]
    for a, b, start in sorted(todo, key=lambda t: t[2] / t[0].shape[0]):
        rs = pl.ds(start, ROWS)
        pltpu.make_async_copy(a.at[rs], b.at[rs], sem.at[0]).start()
    for a, b in zip(ins, outs):
        pltpu.make_async_copy(a, b, sem.at[0]).wait()


def solution(mesh):
    n = mesh.shape["tp"]

    def step(x, dy, pre, w_in, w_down):
        (size, d), ff = x.shape, pre.shape[1]
        half = size // 2
        any_space = pl.BlockSpec(memory_space=pl.ANY)
        shapes = ((size, d), (d, ff), (ff, d))
        dma = pltpu.SemaphoreType.DMA
        outs = pl.pallas_call(
            functools.partial(kernel, n),
            out_shape=[pltpu.VMEM(s, BF16) for s in shapes]
            + [
                jax.ShapeDtypeStruct(s, BF16)
                for s in ((n, size, d), (n, size, d))
            ],
            in_specs=[any_space] * 5,
            out_specs=[pl.BlockSpec(memory_space=pltpu.VMEM)] * 3 + [any_space] * 2,
            scratch_shapes=[
                pltpu.VMEM((d, ff), F32),
                pltpu.VMEM((ff, d), F32),
                pltpu.VMEM((PAIRS, size, ff), BF16),
                pltpu.VMEM((4, half, d), F32),
                pltpu.VMEM((4, half, d), BF16),
                pltpu.VMEM((2, size, d), BF16),
                pltpu.VMEM((2, size, ff), BF16),
                pltpu.VMEM((size, ff), BF16),
                pltpu.VMEM((2, half, d), BF16),
                pltpu.VMEM((4, half, d), BF16),
                pltpu.VMEM((2, half, d), BF16),
                dma((2,)), dma((4,)), dma((2,)), dma((1,)), dma((2,)), dma((1,)), dma((2,)), dma((2,)),
            ],
            compiler_params=pltpu.CompilerParams(collective_id=0, has_side_effects=True, vmem_limit_bytes=VMEM_LIMIT),
            name="mlp_backward",
        )(x, dy, pre, w_in, w_down)
        return tuple(
            pl.pallas_call(
                results,
                out_shape=[jax.ShapeDtypeStruct(s, BF16) for s in shapes],
                in_specs=[pl.BlockSpec(memory_space=pltpu.VMEM)] * 3,
                out_specs=[any_space] * 3,
                scratch_shapes=[dma((1,))],
                compiler_params=pltpu.CompilerParams(vmem_limit_bytes=2**20),
                name="results",
            )(*(pltpu.with_memory_space_constraint(o, pltpu.VMEM) for o in outs[:3]))
        )

    rows = P(("dp", "tp"), None)
    return jax.shard_map(
        step,
        mesh=mesh,
        in_specs=(rows, rows, P("dp", "tp"), P(None, "tp"), P("tp", None)),
        out_specs=(rows, P("dp", "tp"), rows),
        check_vma=False,
    )
```
